32 devices in a mesh: dp: 4 (over y, core), lat: 4 (over z), chan: 2 (over x).
Axes of the slice: x: 2, y: 2, z: 4, core: 2. Of those that a mesh axis runs over, the one named last changes fastest.
Arguments:
- saved_input: bfloat16 [4, 16, 720, 1024], P('dp', None, 'lat', 'chan'), may hold values from -6 to 6
- grad_output: bfloat16 [4, 16, 720, 1024], P('dp', None, 'lat', 'chan'), may hold values from -6 to 6
- legendre: bfloat16 [16, 192, 720], P('lat'), may hold values from -0.21875 to 0.21875
- quad_weight: float32 [720], replicated, may hold values from 0.3 to 3
- mixing_weight: bfloat16 [192, 512, 1024], P('lat', None, 'chan'), may hold values from -0.375 to 0.375
Outputs:
- grad_weight: bfloat16 [192, 512, 1024], P('lat', 'dp', 'chan')
- grad_input: bfloat16 [4, 16, 720, 1024], P('dp', None, 'lat', 'chan')
The draws below stay inside these ranges and needn't reach their ends.
All inputs are finite; a program needn't handle non-finite values.
Results may differ from the reference program's by a relative error of at most 0.014.
Values may be sent and summed in bfloat16 or wider, within the bound.
A program may use at most 192 MiB of HBM per device.

```python
import math
import jax
import jax.numpy as jnp
from jax import lax

NLAT = 720
L = 192
C = 512
BATCH = 4
M = 16
N_DP = 4
N_CHAN = 2


def strengthened(result, rng, source, target, blocks, factor):
    def block_of(axis_at):
        return (jnp.arange(result.shape[axis_at]) // (result.shape[axis_at] // blocks)).reshape((-1,) + (1,) * (result.ndim - 1 - axis_at))

    first = jax.random.permutation(rng, blocks)[block_of(target)]
    other_side = (block_of(target) + blocks // 2) % blocks
    return jnp.where((block_of(source) == first) | (block_of(source) == other_side), factor * result, result)


def level_of(rng, extent, split, low, top_value):
    def one(axis_at, blocks):
        draws = jax.random.uniform(jax.random.fold_in(jax.random.fold_in(rng, 6), axis_at), (blocks,), jnp.float32, low / len(split), top_value / len(split))
        return jnp.repeat(jnp.exp(draws), extent[axis_at] // blocks).reshape((-1,) + (1,) * (len(extent) - axis_at - 1))

    gain = one(*split[0])
    for cut in split[1:]:
        gain = gain * one(*cut)
    return gain


def gaussian(key, shape, scale, limit, shards=(), held_as=jnp.bfloat16):
    factor_of = level_of(key, shape, shards, -0.22, 0.18) if shards else 1.0
    values = jax.random.normal(key, shape, jnp.float32) * scale * factor_of
    return jnp.minimum(jnp.maximum(values, -limit), limit).astype(held_as)


def bell_draw_with(stream_key, extent, deviation, limit, split, heavy, dtype=jnp.bfloat16):
    values = deviation * jax.random.normal(stream_key, extent, jnp.float32)
    if split:
        values = values * level_of(stream_key, extent, split, -0.22, 0.18)
    return jnp.clip(strengthened(values, jax.random.fold_in(stream_key, 3), *heavy), -limit, limit).astype(dtype)


def setup_inputs(seed: int = 0) -> dict:
    key_list = jax.random.split(jax.random.key(seed), 6)
    saved_input = bell_draw_with(key_list[0], (BATCH, M, NLAT, 2 * C), 1.0, 6.0, ((0, 4), (2, 4), (3, 2)), (0, 3, 4, 2.0))
    grad_output = gaussian(key_list[1], (BATCH, M, NLAT, 2 * C), 1.0, 6.0, ((0, 4), (2, 4), (3, 2)))
    legendre = gaussian(key_list[2], (M, L, NLAT), NLAT ** -0.5, 0.21875, ((0, 4),))
    quad_weight = jnp.clip(jnp.exp(jax.random.uniform(key_list[3], (NLAT,), jnp.float32, math.log(0.3), math.log(3.0))), 0.3, 3.0)
    mixing_weight = bell_draw_with(key_list[4], (L, C, 2 * C), C ** -0.5, 0.375, ((0, 4), (2, 2)), (2, 1, 2, 2.0))
    return {"saved_input": saved_input, "grad_output": grad_output, "legendre": legendre, "quad_weight": quad_weight, "mixing_weight": mixing_weight}


def partner_of(grads):
    pairs = grads.reshape(grads.shape[:-1] + (grads.shape[-1] // 2, 2))
    swapped = jnp.stack([pairs[..., 1], -pairs[..., 0]], axis=-1)
    return swapped.reshape(grads.shape)


def weight_terms(spectra, grads):
    pairs = spectra.reshape(spectra.shape[:-1] + (spectra.shape[-1] // 2, 2))
    partner = partner_of(grads)
    first = jnp.einsum('bmli,bmlq->liq', pairs[..., 0], grads)
    second = jnp.einsum('bmli,bmlq->liq', pairs[..., 1], partner)
    return first + second


def reference(saved_input, grad_output, legendre, quad_weight, mixing_weight):
    analysis = (legendre.astype(jnp.float32) * quad_weight[None, None, :]).astype(jnp.bfloat16)
    analysis_wide = analysis.astype(jnp.float32)
    spectra = jnp.einsum('mlj,bmjq->bmlq', analysis_wide, saved_input.astype(jnp.float32)).astype(jnp.bfloat16)
    grad_spectra = jnp.einsum('mlj,bmjq->bmlq', legendre.astype(jnp.float32), grad_output.astype(jnp.float32)).astype(jnp.bfloat16)
    batch = saved_input.shape[0]
    spec_wide = spectra.astype(jnp.float32)
    grad_wide = grad_spectra.astype(jnp.float32)
    spec_groups = spec_wide.reshape((N_DP, batch // N_DP) + spec_wide.shape[1:])
    grad_groups = grad_wide.reshape((N_DP, batch // N_DP) + grad_wide.shape[1:])

    def add_group(running, members):
        term = weight_terms(members[0], members[1]) / batch
        rounded = lax.optimization_barrier(term.astype(jnp.bfloat16))
        return running + rounded.astype(jnp.float32), None

    initial = jnp.zeros(mixing_weight.shape, jnp.float32)
    summed, unused = lax.scan(add_group, initial, (spec_groups, grad_groups))
    grad_weight = summed.astype(jnp.bfloat16)

    width = 2 * C // N_CHAN
    partner_wide = partner_of(grad_wide)
    grad_blocks = jnp.moveaxis(grad_wide.reshape(grad_wide.shape[:3] + (N_CHAN, width)), 3, 0)
    partner_blocks = jnp.moveaxis(partner_wide.reshape(partner_wide.shape[:3] + (N_CHAN, width)), 3, 0)
    weight_wide = mixing_weight.astype(jnp.float32)
    weight_blocks = jnp.moveaxis(weight_wide.reshape(weight_wide.shape[:2] + (N_CHAN, width)), 2, 0)

    def add_block(running, members):
        grads_block, partner_block, weights_block = members
        sum_real = jnp.einsum('bmlq,liq->bmli', grads_block, weights_block)
        sum_imag = jnp.einsum('bmlq,liq->bmli', partner_block, weights_block)
        term = jnp.stack([sum_real, sum_imag], axis=-1).reshape(running.shape)
        rounded = lax.optimization_barrier(term.astype(jnp.bfloat16))
        return running + rounded.astype(jnp.float32), None

    start_sum = jnp.zeros(spec_wide.shape, jnp.float32)
    spec_sum, unused_two = lax.scan(add_block, start_sum, (grad_blocks, partner_blocks, weight_blocks))
    grad_spec_in = spec_sum.astype(jnp.bfloat16)
    grad_input = jnp.einsum('mlj,bmlq->bmjq', analysis_wide, grad_spec_in.astype(jnp.float32)).astype(jnp.bfloat16)
    return (grad_weight, grad_input)
```

```python
import functools
import jax
import jax.numpy as jnp
from jax import lax
from jax.experimental import pallas as pl
from jax.experimental.pallas import tpu as pltpu
from jax.sharding import PartitionSpec as P

BF = jnp.bfloat16
F32 = jnp.float32
MESH = pl.DeviceIdType.MESH


def loop(n, body, unroll=1):
    if n % unroll:
        unroll = 1

    def some(i, carry):
        for j in range(unroll):
            body(i * unroll + j)
        return carry

    lax.fori_loop(0, n // unroll, some, 0)


def nn(a, b):
    return lax.dot_general(a, b, (((1,), (0,)), ((), ())), preferred_element_type=F32)


def nt(a, b):
    return lax.dot_general(a, b, (((1,), (1,)), ((), ())), preferred_element_type=F32)


def tn(a, b):
    return lax.dot_general(a, b, (((0,), (0,)), ((), ())), preferred_element_type=F32)


def put(ref, at, value):
    for i in range(ref.shape[0]):
        ref[i, at, :] = value[:, i * 128:(i + 1) * 128]


def take(ref, start, size, stride):
    at = pl.ds(start, size, stride=stride)
    return jnp.concatenate([ref[i, at, :].astype(BF) for i in range(ref.shape[0])], axis=1)


def partner_rows(x):
    width = x.shape[-1]
    lane = lax.broadcasted_iota(jnp.int32, x.shape, 1)
    ahead, behind = pltpu.roll(x, width - 1, 1), pltpu.roll(x, 1, 1)
    return jnp.where(lane % 2 == 0, ahead, -behind)


def layer_kernel(
    dims,
    leg_hbm, quad_hbm, g_hbm, x_hbm, w_hbm,
    gi_hbm, e_hbm, l_hbm,
    leg, tab, quad, raw, wide, table, pg, ps, rgp, rgm, rsp, rsm,
    tall, flat, keep, give, got, spec, planar, rows16, wbuf, split, join, outb,
    load_sem, w_sem, zs_sem, zr_sem, xs_sem, xr_sem, cs_sem, cr_sem,
    gps, gpr, gms, gmr, sps, spr, sms, smr,
    ts_sem, tr_sem, aps, apr, ams, amr, es_sem, er_sem, el_sem, ps_sem, pr_sem, pl_sem, out_sem,
):
    J, M, Q, L, LB, OM, Z, NDP, NCH, K, KB, WL, WS = dims
    half = Q // 2
    z, c, d = lax.axis_index("lat"), lax.axis_index("chan"), lax.axis_index("dp")
    core = d % 2
    mate, other = d + 1 - 2 * core, 1 - c
    per = OM // (2 * NCH)

    def load(src, dst, i):
        return pltpu.make_async_copy(src, dst, load_sem.at[i])

    loads = [load(leg_hbm, leg, 0), load(g_hbm, raw.at[0], 1), load(x_hbm, raw.at[1], 2),
             load(quad_hbm, quad, 3)]
    for copy in loads:
        copy.start()

    def w_copy(i, slot):
        return pltpu.make_async_copy(w_hbm.at[pl.ds(i * WL, WL)], wbuf.at[slot], w_sem.at[slot])

    for i in range(WS):
        w_copy(i, i).start()

    barrier = pltpu.get_barrier_semaphore()
    for i in range(1, Z):
        pl.semaphore_signal(barrier, inc=1, device_id={"lat": (z + i) % Z}, device_id_type=MESH)
    for i in range(NDP):
        for j in range(NCH):
            if i or j:
                pl.semaphore_signal(
                    barrier, inc=1, device_id={"dp": (d + i) % NDP, "chan": (c + j) % NCH},
                    device_id_type=MESH)

    loads[0].wait()

    def cut(i):
        whole = leg[i]
        for t in range(Z):
            tab[t, i] = whole[:, t * J:(t + 1) * J]

    loop(OM, cut)

    def own_table(i):
        table[z * OM + i] = tab[z, i]

    loop(OM, own_table)
    loads[1].wait()
    JB = 12 if J % 12 == 0 else 1

    def spread(which):
        def body(i):
            block = raw[which, pl.ds(i * JB, JB)]
            put(wide, pl.ds(i * JB * M, JB * M), block.astype(F32).reshape(JB * M, Q))
        loop(J // JB, body)

    def rows_of(m):
        return take(wide, m, J, M)

    spread(0)

    def grad_part(m):
        pg[m] = nn(table[m], rows_of(m)).astype(BF)

    pl.semaphore_wait(barrier, Z - 1 + NDP * NCH - 1)

    mine_q = c * 2 + core

    def z_copy(target, source):
        return pltpu.make_async_remote_copy(
            src_ref=tab.at[target, pl.ds(mine_q * per, per)],
            dst_ref=table.at[pl.ds(source * OM + mine_q * per, per)],
            send_sem=zs_sem.at[target], recv_sem=zr_sem.at[source],
            device_id={"lat": target}, device_id_type=MESH)

    def quarter(owner, q, sends, recvs, where):
        part = table.at[pl.ds(owner * OM + q * per, per)]
        return pltpu.make_async_remote_copy(
            src_ref=part, dst_ref=part, send_sem=sends, recv_sem=recvs,
            device_id=where, device_id_type=MESH)

    def line_steps(p, rp, rm, sends_p, recvs_p, sends_m, recvs_m, region):
        def copy_p(s, t):
            r = region(s, t)
            return pltpu.make_async_remote_copy(
                src_ref=p.at[r], dst_ref=rp.at[r], send_sem=sends_p.at[s, t],
                recv_sem=recvs_p.at[s, t], device_id={"lat": (z + 1) % Z}, device_id_type=MESH)

        def copy_m(s, t):
            r = region(s, t)
            return pltpu.make_async_remote_copy(
                src_ref=p.at[r], dst_ref=rm.at[r], send_sem=sends_m.at[s, t],
                recv_sem=recvs_m.at[s, t], device_id={"lat": (z + Z - 1) % Z}, device_id_type=MESH)

        return copy_p, copy_m

    def g_region(s, t):
        return (pl.ds(s * OM, OM), pl.ds(t * LB, LB), slice(None))

    def s_region(k, t):
        return (slice(None), pl.ds(t * LB + k * KB, KB), slice(None))

    g_p, g_m = line_steps(pg, rgp, rgm, gps, gpr, gms, gmr, g_region)
    s_p, s_m = line_steps(ps, rsp, rsm, sps, spr, sms, smr, s_region)

    def add_g(r, s, t):
        def body(i):
            at = (s * OM + i, pl.ds(t * LB, LB), slice(None))
            pg[at] = (pg[at].astype(F32) + r[at].astype(F32)).astype(BF)
        loop(OM, body)

    def add_s(r, k, t):
        def body(i):
            at = (i, pl.ds(t * LB + k * KB, KB), slice(None))
            ps[at] = (ps[at].astype(F32) + r[at].astype(F32)).astype(BF)
        loop(M, body)

    first, last = z == 0, z == Z - 1

    for i in range(1, Z):
        z_copy((z + Z - i) % Z, z).start()
    loop(OM, lambda i: grad_part(z * OM + i))

    @pl.when(first)
    def _():
        for t in range(Z - 1, 0, -1):
            g_p(0, t).start()

    @pl.when(last)
    def _():
        for t in range(Z - 1):
            g_m(Z - 1, t).start()

    for i in range(1, Z):
        source = (z + i) % Z
        z_copy(z, source).wait_recv()
        quarter(source, mine_q, xs_sem.at[source], xr_sem.at[source], {"chan": other}).start()
        quarter(source, mine_q, cs_sem.at[source, 0], cr_sem.at[source, 0], {"dp": mate}).start()
    for i in range(1, Z):
        source = (z + i) % Z
        x_q = other * 2 + core
        quarter(source, x_q, xs_sem.at[source], xr_sem.at[source], {"chan": other}).wait_recv()
        quarter(source, x_q, cs_sem.at[source, 1], cr_sem.at[source, 1], {"dp": mate}).start()
    for i in range(1, Z):
        source = (z + i) % Z
        quarter(source, c * 2 + 1 - core, cs_sem.at[source, 0], cr_sem.at[source, 0], {"dp": mate}).wait_recv()
        quarter(source, other * 2 + 1 - core, cs_sem.at[source, 1], cr_sem.at[source, 1], {"dp": mate}).wait_recv()
        loop(OM, lambda i: grad_part(source * OM + i))

    def clear(r):
        def body(i):
            r[i, pl.ds(z * LB, LB), :] = jnp.zeros((LB, Q), BF)
        loop(M, body)

    @pl.when(first)
    def _():
        clear(rgp)
        clear(rsp)

    @pl.when(last)
    def _():
        clear(rgm)
        clear(rsm)

    def order(u):
        v = u - (Z - 1)
        early = u < Z - 1
        return jnp.where(early, 0, 1 + v % (Z - 1)), jnp.where(early, Z - 1 - u, Z - 1 - v // (Z - 1))

    pieces = Z * (Z - 1)

    def g_ends(u):
        s, t = order(u)

        @pl.when(first)
        def _():
            g_p(s, t).start()

        @pl.when(last)
        def _():
            g_m(Z - 1 - s, Z - 1 - t).start()

    lax.fori_loop(Z - 1, pieces, lambda u, v: (g_ends(u), v)[1], 0)

    def g_step(u):
        s, t = order(u)
        back, low = Z - 1 - s, Z - 1 - t

        @pl.when((z > 0) & (t > z))
        def _():
            g_p(s, t).wait_recv()
            add_g(rgp, s, t)
            g_p(s, t).start()

        @pl.when((z < Z - 1) & (low < z))
        def _():
            g_m(back, low).wait_recv()
            add_g(rgm, back, low)
            g_m(back, low).start()

    loop(Z - 1, g_step)

    loads[2].wait()
    loads[3].wait()
    spread(1)

    def input_part(m):
        tall[m] = (table[m].astype(F32) * quad[pl.ds(z, 1), :]).astype(BF)
        ps[m] = nn(tall[m], rows_of(m)).astype(BF)

    loop(M, input_part, 2)

    def s_send(k):
        @pl.when(first)
        def _():
            for t in range(Z - 1, 0, -1):
                s_p(k, t).start()

        @pl.when(last)
        def _():
            for t in range(Z - 1):
                s_m(k, t).start()

    s_send(0)
    lax.fori_loop(Z - 1, pieces, lambda u, v: (g_step(u), v)[1], 0)

    def g_done(s):
        @pl.when(z > 0)
        def _():
            g_p(s, z).wait_recv()

        @pl.when(z < Z - 1)
        def _():
            g_m(s, z).wait_recv()

    row = lax.broadcasted_iota(jnp.int32, (Q, Q), 0)
    col = lax.broadcasted_iota(jnp.int32, (Q, Q), 1)
    side = half // (NDP // NCH)
    chan, part = row // 2, row % 2
    split[...] = jnp.where((chan // side) * 2 * side + part * side + chan % side == col, 1.0, 0.0).astype(BF)
    for i in range(2):
        join[i] = jnp.where(2 * row[:half] + i == col[:half], 1.0, 0.0).astype(BF)

    loop(Z, g_done)

    def sum_g(m):
        at = (m, pl.ds(z * LB, LB), slice(None))
        put(wide, pl.ds(m * LB, LB), pg[at].astype(F32) + rgp[at].astype(F32) + rgm[at].astype(F32))

    loop(M, sum_g, 2)

    def flat_of(l):
        rows = take(wide, l, M, LB)
        flat[l, :M, :] = rows
        flat[l, M:, :] = partner_rows(rows.astype(F32)).astype(BF)

    loop(LB, flat_of, 4)

    def e_copy(i):
        return pltpu.make_async_remote_copy(
            src_ref=flat.at[:, pl.ds(0, M)], dst_ref=e_hbm.at[d], send_sem=es_sem.at[i],
            recv_sem=er_sem.at[d], device_id={"dp": (d + i) % NDP}, device_id_type=MESH)

    def e_recv(b):
        return pltpu.make_async_remote_copy(
            src_ref=flat.at[:, pl.ds(0, M)], dst_ref=e_hbm.at[b], send_sem=es_sem.at[0],
            recv_sem=er_sem.at[b], device_id={"dp": mate}, device_id_type=MESH)

    e_local = pltpu.make_async_copy(flat.at[:, pl.ds(0, M)], e_hbm.at[d], el_sem.at[0])
    e_local.start()

    def t_copy(k):
        rows = pl.ds(k * KB, KB)
        return pltpu.make_async_remote_copy(
            src_ref=give.at[rows], dst_ref=got.at[rows], send_sem=ts_sem.at[k],
            recv_sem=tr_sem.at[k], device_id={"chan": other}, device_id_type=MESH)

    def mix(i):
        slot = i % WS
        w_copy(i, slot).wait()

        def one(j):
            l = i * WL + j
            both = flat[l]
            give[l] = nt(both, wbuf[slot, j, pl.ds(other * half, half), :]).astype(BF)
            keep[l] = nt(both, wbuf[slot, j, pl.ds(c * half, half), :]).astype(BF)

        loop(WL, one)

        @pl.when(i + WS < LB // WL)
        def _():
            w_copy(i + WS, slot).start()

        done = (i + 1) * WL

        @pl.when(done % KB == 0)
        def _():
            t_copy(done // KB - 1).start()

    def s_step(k):
        def body(i):
            up, down = Z - 1 - i, i

            @pl.when((up > z) & (z > 0))
            def _():
                s_p(k, up).wait_recv()
                add_s(rsp, k, up)
                s_p(k, up).start()

            @pl.when((down < z) & (z < Z - 1))
            def _():
                s_m(k, down).wait_recv()
                add_s(rsm, k, down)
                s_m(k, down).start()

        loop(Z - 1, body)

    owners = NDP // NCH
    piece_width = Q // owners

    def p_copy(k, e, j):
        return pltpu.make_async_remote_copy(
            src_ref=planar.at[pl.ds(k * KB, KB), :, pl.ds(e * piece_width, piece_width)],
            dst_ref=l_hbm.at[d, pl.ds(k * KB, KB)],
            send_sem=ps_sem.at[k, e * NCH + j], recv_sem=pr_sem.at[k, d],
            device_id={"dp": c * owners + e, "chan": j}, device_id_type=MESH)

    def p_recv(k, b):
        return pltpu.make_async_remote_copy(
            src_ref=planar.at[pl.ds(k * KB, KB), :, pl.ds(0, piece_width)],
            dst_ref=l_hbm.at[b, pl.ds(k * KB, KB)],
            send_sem=ps_sem.at[k, 0], recv_sem=pr_sem.at[k, b],
            device_id={"dp": mate}, device_id_type=MESH)

    def p_local(k, e):
        return pltpu.make_async_copy(
            planar.at[pl.ds(k * KB, KB), :, pl.ds(e * piece_width, piece_width)],
            l_hbm.at[d, pl.ds(k * KB, KB)], pl_sem.at[k])

    def is_me(e, j):
        return (d == c * owners + e) & (c == j)

    def s_finish(k):
        @pl.when(z > 0)
        def _():
            s_p(k, z).wait_recv()

        @pl.when(z < Z - 1)
        def _():
            s_m(k, z).wait_recv()

        def total(m):
            at = (m, pl.ds(z * LB + k * KB, KB), slice(None))
            put(wide, pl.ds(m * KB, KB), ps[at].astype(F32) + rsp[at].astype(F32) + rsm[at].astype(F32))

        loop(M, total, 2)

        def one(l):
            rows16[pl.ds(l * M, M), :] = take(wide, l, M, KB)

        loop(KB, one, 4)
        planar[pl.ds(k * KB, KB)] = nn(rows16[...], split[...]).astype(BF).reshape(KB, M, Q)
        for e in range(owners):
            for j in range(NCH):
                @pl.when(is_me(e, j))
                def _():
                    p_local(k, e).start()

                @pl.when(jnp.logical_not(is_me(e, j)))
                def _():
                    p_copy(k, e, j).start()

    def a_region(t, k):
        return (slice(None), pl.ds(t * LB + k * KB, KB), slice(None))

    def a_p(t, k):
        part = spec.at[a_region(t, k)]
        return pltpu.make_async_remote_copy(
            src_ref=part, dst_ref=part, send_sem=aps.at[t, k], recv_sem=apr.at[t, k],
            device_id={"lat": (z + 1) % Z}, device_id_type=MESH)

    def a_m(t, k):
        part = spec.at[a_region(t, k)]
        return pltpu.make_async_remote_copy(
            src_ref=part, dst_ref=part, send_sem=ams.at[t, k], recv_sem=amr.at[t, k],
            device_id={"lat": (z + Z - 1) % Z}, device_id_type=MESH)

    def combine(k):
        t_copy(k).wait_recv()
        rows = pl.ds(k * KB, KB)
        total = (keep[rows].astype(F32) + got[rows].astype(F32)).astype(BF)
        real = total[:, :M].reshape(KB * M, half)
        imag = total[:, M:].reshape(KB * M, half)
        put(wide, pl.ds(0, KB * M), nn(real, join[0]) + nn(imag, join[1]))

        def one(m):
            spec[m, pl.ds(z * LB + k * KB, KB), :] = take(wide, m, KB, M)

        loop(M, one, 4)

        @pl.when(z < Z - 1)
        def _():
            a_p(z, k).start()

        @pl.when(z > 0)
        def _():
            a_m(z, k).start()

    def a_step(dist):
        def body(k):
            below, above = z - dist, z + dist

            @pl.when(below >= 0)
            def _():
                a_p(below, k).wait_recv()

                @pl.when(z < Z - 1)
                def _():
                    a_p(below, k).start()

            @pl.when(above < Z)
            def _():
                a_m(above, k).wait_recv()

                @pl.when(z > 0)
                def _():
                    a_m(above, k).start()

        loop(K, body)

    def mix_rows(k):
        lax.fori_loop(k * (KB // WL), (k + 1) * (KB // WL), lambda i, v: (mix(i), v)[1], 0)

    mix_rows(0)
    for k in range(1, K):
        mix_rows(k)
        combine(k - 1)
    for i in range(1, NDP):
        e_copy(i).start()
    combine(K - 1)
    for k in range(1, K):
        s_send(k)
    s_step(0)
    s_finish(0)
    todo = list(range(1, K))
    for dist in range(1, Z):
        a_step(dist)
        if todo and dist < Z - 1:
            k = todo.pop(0)
            s_step(k)
            s_finish(k)

    def back(m):
        put(wide, pl.ds(m, J, stride=M), tn(tall[m], spec[m]))

    loop(M, back, 2)

    def narrow(i):
        at = pl.ds(i * JB, JB)
        rows = pl.ds(i * JB * M, JB * M)
        for q in range(Q // 128):
            outb[at, :, q * 128:(q + 1) * 128] = wide[q, rows, :].reshape(JB, M, 128).astype(BF)

    loop(J // JB, narrow)
    out = pltpu.make_async_copy(outb, gi_hbm, out_sem.at[0])
    out.start()
    for k in todo:
        s_step(k)
        s_finish(k)

    e_local.wait()
    for i in range(1, NDP):
        e_copy(i).wait_send()
        e_recv((d + i) % NDP).wait_recv()
    for k in range(K):
        t_copy(k).wait_send()
        for e in range(owners):
            for j in range(NCH):
                @pl.when(is_me(e, j))
                def _():
                    p_local(k, e).wait()

                @pl.when(jnp.logical_not(is_me(e, j)))
                def _():
                    p_copy(k, e, j).wait_send()
        for b in range(NDP):
            @pl.when(jnp.logical_not((b == d) & (d // owners == c)))
            def _():
                p_recv(k, b).wait_recv()
    for i in range(1, Z):
        source = (z + i) % Z
        z_copy(source, z).wait_send()
        quarter(source, mine_q, xs_sem.at[source], xr_sem.at[source], {"chan": other}).wait_send()
        quarter(source, mine_q, cs_sem.at[source, 0], cr_sem.at[source, 0], {"dp": mate}).wait_send()
        quarter(source, other * 2 + core, cs_sem.at[source, 1], cr_sem.at[source, 1], {"dp": mate}).wait_send()

    def drain_line(i):
        s, t = i // Z, i % Z

        @pl.when((t > z) & (z < Z - 1))
        def _():
            g_p(s, t).wait_send()

        @pl.when((t < z) & (z > 0))
        def _():
            g_m(s, t).wait_send()

    loop(Z * Z, drain_line)

    def drain_rest(i):
        k, t = i // Z, i % Z

        @pl.when(t > z)
        def _():
            s_p(k, t).wait_send()

        @pl.when(t < z)
        def _():
            s_m(k, t).wait_send()

        @pl.when((t <= z) & (z < Z - 1))
        def _():
            a_p(t, k).wait_send()

        @pl.when((t >= z) & (z > 0))
        def _():
            a_m(t, k).wait_send()

    loop(K * Z, drain_rest)
    out.wait()


def weight_kernel(scale, e_ref, l_ref, out_ref):
    n_b, n_l, m, q = e_ref.shape
    side = l_ref.shape[-1] // 2

    for l in range(n_l):
        right = e_ref[:, l].reshape(n_b * m, q)
        left = l_ref[:, l].reshape(n_b * m, 2 * side)
        turned = partner_rows(right.astype(F32)).astype(BF)
        total = tn(jnp.concatenate([left[:, :side], left[:, side:]], axis=0),
                   jnp.concatenate([right, turned], axis=0))
        out_ref[l] = (total * scale).astype(BF)


def fast(saved_input, grad_output, legendre, quad_weight, mixing_weight):
    _, M, J, Q = saved_input.shape
    OM, L, _ = legendre.shape
    Z, NDP, NCH = lax.axis_size("lat"), lax.axis_size("dp"), lax.axis_size("chan")
    LB, NI, _ = mixing_weight.shape
    KB = 16
    K = LB // KB
    WL, WS = 8, 3
    half = Q // 2
    owners = NDP // NCH
    side = half // owners
    dims = (J, M, Q, L, LB, OM, Z, NDP, NCH, K, KB, WL, WS)
    quad = quad_weight.reshape(Z, J)
    g = jnp.transpose(grad_output[0], (1, 0, 2))
    x = jnp.transpose(saved_input[0], (1, 0, 2))
    anyspec = pl.BlockSpec(memory_space=pl.ANY)
    dma = pltpu.SemaphoreType.DMA
    part_shape = pltpu.VMEM((M, L, Q), BF)
    scratch = [
        pltpu.VMEM((OM, L, Z * J), BF), pltpu.VMEM((Z, OM, L, J), BF), pltpu.VMEM((Z, J), F32), pltpu.VMEM((2, J, M, Q), BF),
        pltpu.VMEM((Q // 128, J * M, 128), F32), pltpu.VMEM((M, L, J), BF),
        part_shape, part_shape, part_shape, part_shape, part_shape, part_shape,
        pltpu.VMEM((M, L, J), BF), pltpu.VMEM((LB, 2 * M, Q), BF),
        pltpu.VMEM((LB, 2 * M, half), BF), pltpu.VMEM((LB, 2 * M, half), BF),
        pltpu.VMEM((LB, 2 * M, half), BF), part_shape, pltpu.VMEM((LB, M, Q), BF),
        pltpu.VMEM((KB * M, Q), BF),
        pltpu.VMEM((WS, WL, NI, Q), BF), pltpu.VMEM((Q, Q), BF), pltpu.VMEM((2, half, Q), BF),
        pltpu.VMEM((J, M, Q), BF),
        dma((4,)), dma((WS,)), dma((Z,)), dma((Z,)), dma((Z,)), dma((Z,)), dma((Z, 2)), dma((Z, 2)),
        dma((Z, Z)), dma((Z, Z)), dma((Z, Z)), dma((Z, Z)),
        dma((K, Z)), dma((K, Z)), dma((K, Z)), dma((K, Z)),
        dma((K,)), dma((K,)), dma((Z, K)), dma((Z, K)), dma((Z, K)), dma((Z, K)),
        dma((NDP,)), dma((NDP,)), dma((1,)), dma((K, owners * NCH)), dma((K, NDP)), dma((K,)),
        dma((1,)),
    ]
    gi, e, left = pl.pallas_call(
        functools.partial(layer_kernel, dims),
        out_shape=(
            jax.ShapeDtypeStruct((J, M, Q), BF),
            jax.ShapeDtypeStruct((NDP, LB, M, Q), BF),
            jax.ShapeDtypeStruct((NDP, LB, M, 2 * side), BF),
        ),
        in_specs=[anyspec] * 5,
        out_specs=(anyspec,) * 3,
        scratch_shapes=scratch,
        compiler_params=pltpu.CompilerParams(
            collective_id=0, has_side_effects=True, vmem_limit_bytes=67043328
        ),
        name="layer",
    )(legendre, quad, g, x, mixing_weight)
    WB = 8
    gw = pl.pallas_call(
        functools.partial(weight_kernel, 1.0 / (NDP * saved_input.shape[0])),
        out_shape=jax.ShapeDtypeStruct((LB, side, Q), BF),
        grid=(LB // WB,),
        in_specs=[
            pl.BlockSpec((NDP, WB, M, Q), lambda i: (0, i, 0, 0)),
            pl.BlockSpec((NDP, WB, M, 2 * side), lambda i: (0, i, 0, 0)),
        ],
        out_specs=pl.BlockSpec((WB, side, Q), lambda i: (i, 0, 0)),
        compiler_params=pltpu.CompilerParams(dimension_semantics=("arbitrary",)),
        name="weight",
    )(e, left)
    return gw, jnp.transpose(gi, (1, 0, 2))[None]


def lane_swap(width):
    row = lax.broadcasted_iota(jnp.int32, (width, width), 0)
    col = lax.broadcasted_iota(jnp.int32, (width, width), 1)
    up = (row == col + 1) & (col % 2 == 0)
    down = (col == row + 1) & (row % 2 == 0)
    return (up.astype(F32) - down.astype(F32)).astype(BF)


def to_planes(width):
    row = lax.broadcasted_iota(jnp.int32, (width, width), 0)
    col = lax.broadcasted_iota(jnp.int32, (width, width), 1)
    return ((row // 2 + (row % 2) * (width // 2)) == col).astype(BF)


def lanes(x, matrix):
    return jnp.einsum("...q,qp->...p", x, matrix, preferred_element_type=F32).astype(BF)


def shifted(x, axis, step):
    n = lax.axis_size(axis)
    return lax.ppermute(x, axis, [(i, (i + step) % n) for i in range(n)])


def pick(x, index):
    return lax.dynamic_index_in_dim(x, index, 0, keepdims=False)


def on_device(saved_input, grad_output, legendre, quad_weight, mixing_weight):
    local_lat = saved_input.shape[2]
    width = saved_input.shape[3]
    own_m, n_deg, n_lat = legendre.shape
    lat_size = lax.axis_size("lat")
    n_dp, n_chan = lax.axis_size("dp"), lax.axis_size("chan")
    my_dp, my_chan = lax.axis_index("dp"), lax.axis_index("chan")
    batch = saved_input.shape[0] * n_dp
    swap, planes = lane_swap(width), to_planes(width)

    share = 2 if own_m % 2 == 0 and n_dp % 2 == 0 else 1
    per = own_m // share
    half_of = my_dp % share
    orders = pick(legendre.reshape(share, per * n_deg, n_lat), half_of)
    by_lat = orders.T.reshape(lat_size, local_lat, per * n_deg)
    by_lat = lax.all_to_all(by_lat, "lat", split_axis=0, concat_axis=0, tiled=True)
    held = [by_lat]
    if share == 2:
        other = lax.ppermute(by_lat, "dp", [(i, i ^ 1) for i in range(n_dp)])
        first = half_of == 0
        held = [jnp.where(first, by_lat, other), jnp.where(first, other, by_lat)]
    held = [
        jnp.transpose(x.reshape(lat_size, local_lat, per, n_deg), (0, 2, 3, 1))
        for x in held
    ]
    table = jnp.concatenate(held, axis=1).reshape(lat_size * own_m, n_deg, local_lat)
    weights = lax.dynamic_slice_in_dim(
        quad_weight, lax.axis_index("lat") * local_lat, local_lat
    )
    analysis = (table.astype(F32) * weights[None, None, :]).astype(BF)

    def spectrum(tab, grid):
        part = jnp.einsum("mlj,bmjq->lbmq", tab, grid, preferred_element_type=F32)
        return lax.psum_scatter(part.astype(BF), "lat", scatter_dimension=0, tiled=True)

    grads = spectrum(table, grad_output)
    spectra = spectrum(analysis, saved_input)
    n_l, n_b, n_m = grads.shape[:3]
    rows = n_b * n_m

    flat = grads.reshape(n_l, rows, width)
    both = jnp.concatenate([flat, lanes(flat, swap)], axis=1)
    n_i = mixing_weight.shape[1]
    mine = n_i // n_chan
    split_weight = mixing_weight.reshape(n_l, n_chan, mine, width)
    terms = jnp.einsum("lrq,lciq->clri", both, split_weight, preferred_element_type=F32)
    terms = terms.astype(BF)
    total = pick(terms, my_chan).astype(F32)
    for step in range(1, n_chan):
        sent = pick(terms, (my_chan + step) % n_chan)
        total = total + shifted(sent, "chan", step).astype(F32)
    total = total.astype(BF)
    half = lanes_join(total.reshape(n_l, 2, rows, mine), planes)
    everyone = [flat] + [shifted(flat, "dp", step) for step in range(1, n_dp)]

    spectra, half, *everyone = lax.optimization_barrier((spectra, half, *everyone))
    spec_in = lax.all_gather(half, "lat", axis=0, tiled=True).reshape(-1, n_b, n_m, width)
    grad_input = jnp.einsum(
        "mlj,lbmq->bmjq", analysis, spec_in, preferred_element_type=F32
    ).astype(BF)

    block = n_i // n_dp
    size = min(block, mine)
    per_chan, per_block = mine // size, block // size
    planar = lanes(spectra.reshape(n_l, rows, width), planes)
    pieces = jnp.moveaxis(planar.reshape(n_l, rows, 2, per_chan, size), 3, 0)
    pieces = pieces.reshape(per_chan, n_l, rows, 2 * size)
    pieces = jnp.concatenate(
        [pieces] + [shifted(pieces, "chan", step) for step in range(1, n_chan)]
    )

    def piece(index):
        place = (my_chan - index // per_chan) % n_chan
        return pick(pieces, place * per_chan + index % per_chan)

    def block_of(owner):
        parts = [piece(owner * per_block + t) for t in range(per_block)]
        return jnp.stack(parts)

    ours = [block_of(my_dp)]
    for step in range(1, n_dp):
        ours.append(shifted(block_of((my_dp + step) % n_dp), "dp", step))
    left = jnp.stack(ours).reshape(n_dp, per_block, n_l, rows, 2, size)
    right = jnp.stack(everyone)
    right = jnp.stack([right, lanes(right, swap)])
    grad_weight = jnp.einsum(
        "dtlrpi,pdlrq->ltiq", left, right, preferred_element_type=F32
    ) / batch
    return (grad_weight.reshape(n_l, block, width).astype(BF), grad_input)


def lanes_join(parts, planes):
    n = parts.shape[-1]
    real = jnp.einsum("lri,qi->lrq", parts[:, 0], planes[:, :n], preferred_element_type=F32)
    imag = jnp.einsum("lri,qi->lrq", parts[:, 1], planes[:, n:], preferred_element_type=F32)
    return (real + imag).astype(BF)


def on_slice(saved_input, grad_output, legendre, quad_weight, mixing_weight):
    n_b, n_m, n_j, width = saved_input.shape
    own_m, n_deg, _ = legendre.shape
    lat, n_dp, n_chan = (lax.axis_size(a) for a in ("lat", "dp", "chan"))
    n_l, n_i, _ = mixing_weight.shape
    fits = (
        n_b == 1 and n_chan == 2 and n_dp % 2 == 0 and n_dp // n_chan == 2
        and n_m == lat * own_m and n_m == 16 and own_m % (2 * n_chan) == 0
        and n_l % 16 == 0 and n_l >= 32 and width % 512 == 0 and n_i == width
        and n_j % 12 == 0
    )
    step = fast if fits else on_device
    return step(saved_input, grad_output, legendre, quad_weight, mixing_weight)


def solution(mesh):
    in_specs = (
        P("dp", None, "lat", "chan"),
        P("dp", None, "lat", "chan"),
        P("lat", None, None),
        P(),
        P("lat", None, "chan"),
    )
    out_specs = (P("lat", "dp", "chan"), P("dp", None, "lat", "chan"))
    return jax.shard_map(
        on_slice, mesh=mesh, in_specs=in_specs, out_specs=out_specs, check_vma=False
    )
```

```python
import functools
import jax
import jax.numpy as jnp
from jax import lax
from jax.experimental import pallas as pl
from jax.experimental.pallas import tpu as pltpu
from jax.sharding import PartitionSpec as P

BF = jnp.bfloat16
F32 = jnp.float32
MESH = pl.DeviceIdType.MESH


START = 0
DELAY = 3


def loop(n, body, unroll=1):
    if n % unroll:
        unroll = 1

    def some(i, carry):
        for j in range(unroll):
            body(i * unroll + j)
        return carry

    lax.fori_loop(0, n // unroll, some, 0)


def nn(a, b):
    return lax.dot_general(a, b, (((1,), (0,)), ((), ())), preferred_element_type=F32)


def nt(a, b):
    return lax.dot_general(a, b, (((1,), (1,)), ((), ())), preferred_element_type=F32)


def tn(a, b):
    return lax.dot_general(a, b, (((0,), (0,)), ((), ())), preferred_element_type=F32)


def put(ref, at, value):
    for i in range(ref.shape[0]):
        ref[i, at, :] = value[:, i * 128:(i + 1) * 128]


def take(ref, start, size, stride):
    at = pl.ds(start, size, stride=stride)
    return jnp.concatenate([ref[i, at, :].astype(BF) for i in range(ref.shape[0])], axis=1)


def partner_rows(x):
    width = x.shape[-1]
    lane = lax.broadcasted_iota(jnp.int32, x.shape, 1)
    ahead, behind = pltpu.roll(x, width - 1, 1), pltpu.roll(x, 1, 1)
    return jnp.where(lane % 2 == 0, ahead, -behind)


def layer_kernel(
    dims,
    leg_hbm, quad_hbm, g_hbm, x_hbm, w_hbm,
    gi_hbm, e_hbm, l_hbm,
    leg, tab, quad_in, quad, raw, wide, table, pg, ps, rgp, rgm, rsp, rsm,
    tall, flat, keep, give, got, spec, planar, rows16, wbuf, split, join, outb,
    load_sem, w_sem, zs_sem, zr_sem, xs_sem, xr_sem, cs_sem, cr_sem,
    gps, gpr, gms, gmr, sps, spr, sms, smr,
    ts_sem, tr_sem, aps, apr, ams, amr, es_sem, er_sem, el_sem, ps_sem, pr_sem, pl_sem, out_sem,
):
    J, M, Q, L, LB, OM, Z, NDP, NCH, K, KB, WL, WS = dims
    half = Q // 2
    z, c, d = lax.axis_index("lat"), lax.axis_index("chan"), lax.axis_index("dp")
    core = d % 2
    mate, other = d + 1 - 2 * core, 1 - c
    per = OM // (2 * NCH)

    def load(src, dst, i):
        return pltpu.make_async_copy(src, dst, load_sem.at[i])

    loads = [load(leg_hbm, leg, 0), load(g_hbm, raw.at[0], 1), load(x_hbm, raw.at[1], 2),
             load(quad_hbm, quad_in, 3)]
    for i in (0, 1, 3, 2):
        loads[i].start()

    def w_copy(i, slot):
        return pltpu.make_async_copy(w_hbm.at[pl.ds(i * WL, WL)], wbuf.at[slot], w_sem.at[slot])

    for i in range(WS):
        w_copy(i, i).start()

    barrier = pltpu.get_barrier_semaphore()
    for i in range(1, Z):
        pl.semaphore_signal(barrier, inc=1, device_id={"lat": (z + i) % Z}, device_id_type=MESH)
    for i in range(NDP):
        for j in range(NCH):
            if i or j:
                pl.semaphore_signal(
                    barrier, inc=1, device_id={"dp": (d + i) % NDP, "chan": (c + j) % NCH},
                    device_id_type=MESH)

    loads[0].wait()

    def cut(i):
        whole = leg[i]
        for t in range(Z):
            tab[t, i] = whole[:, t * J:(t + 1) * J]

    loop(OM, cut)

    def own_table(i):
        table[z * OM + i] = tab[z, i]

    loop(OM, own_table)
    loads[1].wait()
    JB = 12 if J % 12 == 0 else 1

    def spread(which):
        def body(i):
            block = raw[which, pl.ds(i * JB, JB)]
            put(wide, pl.ds(i * JB * M, JB * M), block.astype(F32).reshape(JB * M, Q))
        loop(J // JB, body)

    def rows_of(m):
        return take(wide, m, J, M)

    spread(0)

    def grad_part(m):
        pg[m] = nn(table[m], rows_of(m)).astype(BF)

    pl.semaphore_wait(barrier, Z - 1 + NDP * NCH - 1)

    mine_q = c * 2 + core

    def z_copy(target, source):
        return pltpu.make_async_remote_copy(
            src_ref=tab.at[target, pl.ds(mine_q * per, per)],
            dst_ref=table.at[pl.ds(source * OM + mine_q * per, per)],
            send_sem=zs_sem.at[target], recv_sem=zr_sem.at[source],
            device_id={"lat": target}, device_id_type=MESH)

    def quarter(owner, q, sends, recvs, where):
        part = table.at[pl.ds(owner * OM + q * per, per)]
        return pltpu.make_async_remote_copy(
            src_ref=part, dst_ref=part, send_sem=sends, recv_sem=recvs,
            device_id=where, device_id_type=MESH)

    def line_steps(p, rp, rm, sends_p, recvs_p, sends_m, recvs_m, region):
        def copy_p(s, t):
            r = region(s, t)
            return pltpu.make_async_remote_copy(
                src_ref=p.at[r], dst_ref=rp.at[r], send_sem=sends_p.at[s, t],
                recv_sem=recvs_p.at[s, t], device_id={"lat": (z + 1) % Z}, device_id_type=MESH)

        def copy_m(s, t):
            r = region(s, t)
            return pltpu.make_async_remote_copy(
                src_ref=p.at[r], dst_ref=rm.at[r], send_sem=sends_m.at[s, t],
                recv_sem=recvs_m.at[s, t], device_id={"lat": (z + Z - 1) % Z}, device_id_type=MESH)

        return copy_p, copy_m

    def g_region(s, t):
        return (pl.ds(s * OM, OM), pl.ds(t * LB, LB), slice(None))

    def s_region(k, t):
        return (slice(None), pl.ds(t * LB + k * KB, KB), slice(None))

    g_p, g_m = line_steps(pg, rgp, rgm, gps, gpr, gms, gmr, g_region)
    s_p, s_m = line_steps(ps, rsp, rsm, sps, spr, sms, smr, s_region)

    def add_g(r, s, t):
        def body(i):
            at = (s * OM + i, pl.ds(t * LB, LB), slice(None))
            pg[at] = (pg[at].astype(F32) + r[at].astype(F32)).astype(BF)
        loop(OM, body)

    def add_s(r, k, t):
        def body(i):
            at = (i, pl.ds(t * LB + k * KB, KB), slice(None))
            ps[at] = (ps[at].astype(F32) + r[at].astype(F32)).astype(BF)
        loop(M, body)

    first, last = z == 0, z == Z - 1

    for i in range(1, Z):
        z_copy((z + Z - i) % Z, z).start()
    loop(OM, lambda i: grad_part(z * OM + i))

    @pl.when(first)
    def _():
        for t in [*range(Z - 2, 0, -1), Z - 1]:
            g_p(0, t).start()

    @pl.when(last)
    def _():
        for t in [*range(1, Z - 1), 0]:
            g_m(Z - 1, t).start()

    for i in range(1, Z):
        source = (z + i) % Z
        z_copy(z, source).wait_recv()
        quarter(source, mine_q, xs_sem.at[source], xr_sem.at[source], {"chan": other}).start()
        quarter(source, mine_q, cs_sem.at[source, 0], cr_sem.at[source, 0], {"dp": mate}).start()
    for i in range(1, Z):
        source = (z + i) % Z
        x_q = other * 2 + core
        quarter(source, x_q, xs_sem.at[source], xr_sem.at[source], {"chan": other}).wait_recv()
        quarter(source, x_q, cs_sem.at[source, 1], cr_sem.at[source, 1], {"dp": mate}).start()
    for i in range(1, Z):
        source = (z + i) % Z
        quarter(source, c * 2 + 1 - core, cs_sem.at[source, 0], cr_sem.at[source, 0], {"dp": mate}).wait_recv()
        quarter(source, other * 2 + 1 - core, cs_sem.at[source, 1], cr_sem.at[source, 1], {"dp": mate}).wait_recv()
        loop(OM, lambda i: grad_part(source * OM + i))

    def clear(r):
        def body(i):
            r[i, pl.ds(z * LB, LB), :] = jnp.zeros((LB, Q), BF)
        loop(M, body)

    @pl.when(first)
    def _():
        clear(rgp)
        clear(rsp)

    @pl.when(last)
    def _():
        clear(rgm)
        clear(rsm)

    def order(u):
        v = u - (Z - 1)
        early = u < Z - 1
        p = jnp.where(early, u, v // (Z - 1))
        return jnp.where(early, 0, 1 + v % (Z - 1)), jnp.where(p < Z - 2, Z - 2 - p, Z - 1)

    def down_block(t):
        return Z - 1 - t

    pieces = Z * (Z - 1)

    def g_ends(u):
        s, t = order(u)

        @pl.when(first)
        def _():
            g_p(s, t).start()

        @pl.when(last)
        def _():
            g_m(Z - 1 - s, down_block(t)).start()

    lax.fori_loop(Z - 1, pieces, lambda u, v: (g_ends(u), v)[1], 0)

    loads[2].wait()
    loads[3].wait()
    weights = quad_in[...].reshape(1, Z * J)
    for t in range(Z):
        quad[t:t + 1, :] = weights[:, t * J:(t + 1) * J]

    spread(1)

    def input_part(m):
        tall[m] = (table[m].astype(F32) * quad[pl.ds(z, 1), :]).astype(BF)
        ps[m] = nn(tall[m], rows_of(m)).astype(BF)

    loop(M, input_part, 2)

    def s_send(k):
        @pl.when(first)
        def _():
            for t in range(Z - 1, 0, -1):
                s_p(k, t).start()

        @pl.when(last)
        def _():
            for t in range(Z - 1):
                s_m(k, t).start()

    for k in range(K - 1):
        s_send(k)

    def g_done(s):
        @pl.when(z > 0)
        def _():
            g_p(s, z).wait_recv()

        @pl.when(z < Z - 1)
        def _():
            g_m(s, z).wait_recv()

    row = lax.broadcasted_iota(jnp.int32, (Q, Q), 0)
    col = lax.broadcasted_iota(jnp.int32, (Q, Q), 1)
    side = half // (NDP // NCH)
    chan, part = row // 2, row % 2
    split[...] = jnp.where((chan // side) * 2 * side + part * side + chan % side == col, 1.0, 0.0).astype(BF)
    for i in range(2):
        join[i] = jnp.where(2 * row[:half] + i == col[:half], 1.0, 0.0).astype(BF)

    def sum_g(m):
        at = (m, pl.ds(z * LB, LB), slice(None))
        put(wide, pl.ds(m * LB, LB), pg[at].astype(F32) + rgp[at].astype(F32) + rgm[at].astype(F32))


    def flat_of(l):
        rows = take(wide, l, M, LB)
        flat[l, :M, :] = rows
        flat[l, M:, :] = partner_rows(rows.astype(F32)).astype(BF)


    def e_copy(i):
        return pltpu.make_async_remote_copy(
            src_ref=flat.at[:, pl.ds(0, M)], dst_ref=e_hbm.at[d], send_sem=es_sem.at[i],
            recv_sem=er_sem.at[d], device_id={"dp": (d + i) % NDP}, device_id_type=MESH)

    def e_recv(b):
        return pltpu.make_async_remote_copy(
            src_ref=flat.at[:, pl.ds(0, M)], dst_ref=e_hbm.at[b], send_sem=es_sem.at[0],
            recv_sem=er_sem.at[b], device_id={"dp": mate}, device_id_type=MESH)

    e_local = pltpu.make_async_copy(flat.at[:, pl.ds(0, M)], e_hbm.at[d], el_sem.at[0])

    def own_spectra():
        loop(Z, g_done)
        loop(M, sum_g, 2)
        loop(LB, flat_of, 4)
        e_local.start()
        for i in range(1, NDP):
            e_copy(i).start()

    def t_copy(k):
        rows = pl.ds(k * KB, KB)
        return pltpu.make_async_remote_copy(
            src_ref=give.at[rows], dst_ref=got.at[rows], send_sem=ts_sem.at[k],
            recv_sem=tr_sem.at[k], device_id={"chan": other}, device_id_type=MESH)

    def mix(i):
        slot = i % WS
        w_copy(i, slot).wait()

        def one(j):
            l = i * WL + j
            both = flat[l]
            give[l] = nt(both, wbuf[slot, j, pl.ds(other * half, half), :]).astype(BF)
            keep[l] = nt(both, wbuf[slot, j, pl.ds(c * half, half), :]).astype(BF)

        loop(WL, one)

        @pl.when(i + WS < LB // WL)
        def _():
            w_copy(i + WS, slot).start()

        done = (i + 1) * WL

        @pl.when(done % KB == 0)
        def _():
            t_copy(done // KB - 1).start()

    owners = NDP // NCH
    piece_width = Q // owners

    def p_copy(k, e, j):
        return pltpu.make_async_remote_copy(
            src_ref=planar.at[pl.ds(k * KB, KB), :, pl.ds(e * piece_width, piece_width)],
            dst_ref=l_hbm.at[d, pl.ds(k * KB, KB)],
            send_sem=ps_sem.at[k, e * NCH + j], recv_sem=pr_sem.at[k, d],
            device_id={"dp": c * owners + e, "chan": j}, device_id_type=MESH)

    def p_recv(k, b):
        return pltpu.make_async_remote_copy(
            src_ref=planar.at[pl.ds(k * KB, KB), :, pl.ds(0, piece_width)],
            dst_ref=l_hbm.at[b, pl.ds(k * KB, KB)],
            send_sem=ps_sem.at[k, 0], recv_sem=pr_sem.at[k, b],
            device_id={"dp": mate}, device_id_type=MESH)

    def p_local(k, e):
        return pltpu.make_async_copy(
            planar.at[pl.ds(k * KB, KB), :, pl.ds(e * piece_width, piece_width)],
            l_hbm.at[d, pl.ds(k * KB, KB)], pl_sem.at[k])

    def is_me(e, j):
        return (d == c * owners + e) & (c == j)

    def s_finish(k):
        @pl.when(z > 0)
        def _():
            s_p(k, z).wait_recv()

        @pl.when(z < Z - 1)
        def _():
            s_m(k, z).wait_recv()

        def total(m):
            at = (m, pl.ds(z * LB + k * KB, KB), slice(None))
            put(wide, pl.ds(m * KB, KB), ps[at].astype(F32) + rsp[at].astype(F32) + rsm[at].astype(F32))

        loop(M, total, 2)

        def one(l):
            rows16[pl.ds(l * M, M), :] = take(wide, l, M, KB)

        loop(KB, one, 4)
        planar[pl.ds(k * KB, KB)] = nn(rows16[...], split[...]).astype(BF).reshape(KB, M, Q)
        for e in range(owners):
            for j in range(NCH):
                @pl.when(is_me(e, j))
                def _():
                    p_local(k, e).start()

                @pl.when(jnp.logical_not(is_me(e, j)))
                def _():
                    p_copy(k, e, j).start()

    def a_region(t, k):
        return (slice(None), pl.ds(t * LB + k * KB, KB), slice(None))

    def a_p(t, k):
        part = spec.at[a_region(t, k)]
        return pltpu.make_async_remote_copy(
            src_ref=part, dst_ref=part, send_sem=aps.at[t, k], recv_sem=apr.at[t, k],
            device_id={"lat": (z + 1) % Z}, device_id_type=MESH)

    def a_m(t, k):
        part = spec.at[a_region(t, k)]
        return pltpu.make_async_remote_copy(
            src_ref=part, dst_ref=part, send_sem=ams.at[t, k], recv_sem=amr.at[t, k],
            device_id={"lat": (z + Z - 1) % Z}, device_id_type=MESH)

    def combine(k):
        t_copy(k).wait_recv()
        rows = pl.ds(k * KB, KB)
        total = (keep[rows].astype(F32) + got[rows].astype(F32)).astype(BF)
        real = total[:, :M].reshape(KB * M, half)
        imag = total[:, M:].reshape(KB * M, half)
        put(wide, pl.ds(0, KB * M), nn(real, join[0]) + nn(imag, join[1]))

        def one(m):
            spec[m, pl.ds(z * LB + k * KB, KB), :] = take(wide, m, KB, M)

        loop(M, one, 4)

        @pl.when(z < Z - 1)
        def _():
            a_p(z, k).start()

        @pl.when(z > 0)
        def _():
            a_m(z, k).start()

        @pl.when(k == K - 1)
        def _():
            s_send(K - 1)

    def mix_rows(k):
        lax.fori_loop(k * (KB // WL), (k + 1) * (KB // WL), lambda i, v: (mix(i), v)[1], 0)

    s_count = (K - 1) * (Z - 1)
    gather_at = pieces + s_count
    final_at = gather_at + K
    total_pieces = final_at + Z - 1

    def up(n):
        @pl.when((n >= 0) & (n < pieces))
        def _():
            s, t = order(n)

            @pl.when(t > z)
            def _():
                g_p(s, t).wait_recv()
                add_g(rgp, s, t)
                g_p(s, t).start()

        late = n >= final_at

        @pl.when(((n >= pieces) & (n < gather_at)) | (late & (n < total_pieces)))
        def _():
            v = jnp.where(late, n - final_at + s_count, n - pieces)
            k, t = v // (Z - 1), Z - 1 - v % (Z - 1)

            @pl.when(t > z)
            def _():
                s_p(k, t).wait_recv()
                add_s(rsp, k, t)
                s_p(k, t).start()

        @pl.when((n >= gather_at) & (n < final_at))
        def _():
            a_p(0, n - gather_at).wait_recv()
            a_p(0, n - gather_at).start()

    def down(n):
        @pl.when((n >= 0) & (n < pieces))
        def _():
            s, t = order(n)
            s, t = Z - 1 - s, down_block(t)

            @pl.when(t < z)
            def _():
                g_m(s, t).wait_recv()
                add_g(rgm, s, t)
                g_m(s, t).start()

        late = n >= final_at

        @pl.when(((n >= pieces) & (n < gather_at)) | (late & (n < total_pieces)))
        def _():
            v = jnp.where(late, n - final_at + s_count, n - pieces)
            k, t = v // (Z - 1), v % (Z - 1)

            @pl.when(t < z)
            def _():
                s_m(k, t).wait_recv()
                add_s(rsm, k, t)
                s_m(k, t).start()

        @pl.when((n >= gather_at) & (n < final_at))
        def _():
            a_m(Z - 1, n - gather_at).wait_recv()
            a_m(Z - 1, n - gather_at).start()

    inner = jnp.logical_not(first | last)
    begin = (Z - 1) * (Z - 1) + START - 1
    ready = [pieces + (k + 1) * (Z - 1) + 1 for k in range(K - 1)]

    def slot(v):
        @pl.when(inner)
        def _():
            up(v - (z - 1))
            down(v - (Z - 2 - z))

        u = v - begin

        @pl.when(u == 0)
        def _():
            own_spectra()

        @pl.when((u >= 1) & (u < K + 1))
        def _():
            mix_rows(u - 1)

        @pl.when((u >= K) & (u < 2 * K))
        def _():
            combine(u - K)

        for b in range(1, Z - 1):
            @pl.when((b < z) & inner)
            def _():
                w = v - begin - (K - 1) - DELAY * (z - b)

                @pl.when((w >= 0) & (w < K))
                def _():
                    a_p(b, w).wait_recv()
                    a_p(b, w).start()

            @pl.when((b > z) & inner)
            def _():
                w = v - begin - (K - 1) - DELAY * (b - z)

                @pl.when((w >= 0) & (w < K))
                def _():
                    a_m(b, w).wait_recv()
                    a_m(b, w).start()

        hit = functools.reduce(lambda a, b: a | b, [v == r for r in ready])

        @pl.when(hit)
        def _():
            s_finish((v - ready[0]) // (Z - 1))

    loop(total_pieces + Z - 2, slot)

    def collect(i):
        b, k = i // K, i % K

        @pl.when(last & (b < Z - 1))
        def _():
            a_p(b, k).wait_recv()

        @pl.when(first & (b > 0))
        def _():
            a_m(b, k).wait_recv()

    s_finish(K - 1)
    loop(Z * K, collect)

    def back(m):
        put(wide, pl.ds(m, J, stride=M), tn(tall[m], spec[m]))

    loop(M, back, 2)

    def narrow(i):
        at = pl.ds(i * JB, JB)
        rows = pl.ds(i * JB * M, JB * M)
        for q in range(Q // 128):
            outb[at, :, q * 128:(q + 1) * 128] = wide[q, rows, :].reshape(JB, M, 128).astype(BF)

    loop(J // JB, narrow)
    out = pltpu.make_async_copy(outb, gi_hbm, out_sem.at[0])
    out.start()
    e_local.wait()
    for i in range(1, NDP):
        e_copy(i).wait_send()
        e_recv((d + i) % NDP).wait_recv()
    for k in range(K):
        t_copy(k).wait_send()
        for e in range(owners):
            for j in range(NCH):
                @pl.when(is_me(e, j))
                def _():
                    p_local(k, e).wait()

                @pl.when(jnp.logical_not(is_me(e, j)))
                def _():
                    p_copy(k, e, j).wait_send()
        for b in range(NDP):
            @pl.when(jnp.logical_not((b == d) & (d // owners == c)))
            def _():
                p_recv(k, b).wait_recv()
    for i in range(1, Z):
        source = (z + i) % Z
        z_copy(source, z).wait_send()
        quarter(source, mine_q, xs_sem.at[source], xr_sem.at[source], {"chan": other}).wait_send()
        quarter(source, mine_q, cs_sem.at[source, 0], cr_sem.at[source, 0], {"dp": mate}).wait_send()
        quarter(source, other * 2 + core, cs_sem.at[source, 1], cr_sem.at[source, 1], {"dp": mate}).wait_send()

    def drain_line(i):
        s, t = i // Z, i % Z

        @pl.when((t > z) & (z < Z - 1))
        def _():
            g_p(s, t).wait_send()

        @pl.when((t < z) & (z > 0))
        def _():
            g_m(s, t).wait_send()

    loop(Z * Z, drain_line)

    def drain_rest(i):
        k, t = i // Z, i % Z

        @pl.when(t > z)
        def _():
            s_p(k, t).wait_send()

        @pl.when(t < z)
        def _():
            s_m(k, t).wait_send()

        @pl.when((t <= z) & (z < Z - 1))
        def _():
            a_p(t, k).wait_send()

        @pl.when((t >= z) & (z > 0))
        def _():
            a_m(t, k).wait_send()

    loop(K * Z, drain_rest)
    out.wait()


def weight_kernel(scale, e_ref, l_ref, out_ref):
    n_b, n_l, m, q = e_ref.shape
    side = l_ref.shape[-1] // 2

    for l in range(n_l):
        right = e_ref[:, l].reshape(n_b * m, q)
        left = l_ref[:, l].reshape(n_b * m, 2 * side)
        turned = partner_rows(right.astype(F32)).astype(BF)
        total = tn(jnp.concatenate([left[:, :side], left[:, side:]], axis=0),
                   jnp.concatenate([right, turned], axis=0))
        out_ref[l] = (total * scale).astype(BF)


def fast(saved_input, grad_output, legendre, quad_weight, mixing_weight):
    _, M, J, Q = saved_input.shape
    OM, L, _ = legendre.shape
    Z, NDP, NCH = lax.axis_size("lat"), lax.axis_size("dp"), lax.axis_size("chan")
    LB, NI, _ = mixing_weight.shape
    KB = 16
    K = LB // KB
    WL, WS = 8, 3
    half = Q // 2
    owners = NDP // NCH
    side = half // owners
    dims = (J, M, Q, L, LB, OM, Z, NDP, NCH, K, KB, WL, WS)
    quad = quad_weight
    g = jnp.transpose(grad_output[0], (1, 0, 2))
    x = jnp.transpose(saved_input[0], (1, 0, 2))
    anyspec = pl.BlockSpec(memory_space=pl.ANY)
    dma = pltpu.SemaphoreType.DMA
    part_shape = pltpu.VMEM((M, L, Q), BF)
    scratch = [
        pltpu.VMEM((OM, L, Z * J), BF), pltpu.VMEM((Z, OM, L, J), BF), pltpu.VMEM((Z * J,), F32), pltpu.VMEM((Z, J), F32), pltpu.VMEM((2, J, M, Q), BF),
        pltpu.VMEM((Q // 128, J * M, 128), F32), pltpu.VMEM((M, L, J), BF),
        part_shape, part_shape, part_shape, part_shape, part_shape, part_shape,
        pltpu.VMEM((M, L, J), BF), pltpu.VMEM((LB, 2 * M, Q), BF),
        pltpu.VMEM((LB, 2 * M, half), BF), pltpu.VMEM((LB, 2 * M, half), BF),
        pltpu.VMEM((LB, 2 * M, half), BF), part_shape, pltpu.VMEM((LB, M, Q), BF),
        pltpu.VMEM((KB * M, Q), BF),
        pltpu.VMEM((WS, WL, NI, Q), BF), pltpu.VMEM((Q, Q), BF), pltpu.VMEM((2, half, Q), BF),
        pltpu.VMEM((J, M, Q), BF),
        dma((4,)), dma((WS,)), dma((Z,)), dma((Z,)), dma((Z,)), dma((Z,)), dma((Z, 2)), dma((Z, 2)),
        dma((Z, Z)), dma((Z, Z)), dma((Z, Z)), dma((Z, Z)),
        dma((K, Z)), dma((K, Z)), dma((K, Z)), dma((K, Z)),
        dma((K,)), dma((K,)), dma((Z, K)), dma((Z, K)), dma((Z, K)), dma((Z, K)),
        dma((NDP,)), dma((NDP,)), dma((1,)), dma((K, owners * NCH)), dma((K, NDP)), dma((K,)),
        dma((1,)),
    ]
    gi, e, left = pl.pallas_call(
        functools.partial(layer_kernel, dims),
        out_shape=(
            jax.ShapeDtypeStruct((J, M, Q), BF),
            jax.ShapeDtypeStruct((NDP, LB, M, Q), BF),
            jax.ShapeDtypeStruct((NDP, LB, M, 2 * side), BF),
        ),
        in_specs=[anyspec] * 5,
        out_specs=(anyspec,) * 3,
        scratch_shapes=scratch,
        compiler_params=pltpu.CompilerParams(
            collective_id=0, has_side_effects=True, vmem_limit_bytes=67043328
        ),
        name="layer",
    )(legendre, quad, g, x, mixing_weight)
    WB = 8
    gw = pl.pallas_call(
        functools.partial(weight_kernel, 1.0 / (NDP * saved_input.shape[0])),
        out_shape=jax.ShapeDtypeStruct((LB, side, Q), BF),
        grid=(LB // WB,),
        in_specs=[
            pl.BlockSpec((NDP, WB, M, Q), lambda i: (0, i, 0, 0)),
            pl.BlockSpec((NDP, WB, M, 2 * side), lambda i: (0, i, 0, 0)),
        ],
        out_specs=pl.BlockSpec((WB, side, Q), lambda i: (i, 0, 0)),
        compiler_params=pltpu.CompilerParams(dimension_semantics=("arbitrary",)),
        name="weight",
    )(e, left)
    return gw, jnp.transpose(gi, (1, 0, 2))[None]


def lane_swap(width):
    row = lax.broadcasted_iota(jnp.int32, (width, width), 0)
    col = lax.broadcasted_iota(jnp.int32, (width, width), 1)
    up = (row == col + 1) & (col % 2 == 0)
    down = (col == row + 1) & (row % 2 == 0)
    return (up.astype(F32) - down.astype(F32)).astype(BF)


def to_planes(width):
    row = lax.broadcasted_iota(jnp.int32, (width, width), 0)
    col = lax.broadcasted_iota(jnp.int32, (width, width), 1)
    return ((row // 2 + (row % 2) * (width // 2)) == col).astype(BF)


def lanes(x, matrix):
    return jnp.einsum("...q,qp->...p", x, matrix, preferred_element_type=F32).astype(BF)


def shifted(x, axis, step):
    n = lax.axis_size(axis)
    return lax.ppermute(x, axis, [(i, (i + step) % n) for i in range(n)])


def pick(x, index):
    return lax.dynamic_index_in_dim(x, index, 0, keepdims=False)


def on_device(saved_input, grad_output, legendre, quad_weight, mixing_weight):
    local_lat = saved_input.shape[2]
    width = saved_input.shape[3]
    own_m, n_deg, n_lat = legendre.shape
    lat_size = lax.axis_size("lat")
    n_dp, n_chan = lax.axis_size("dp"), lax.axis_size("chan")
    my_dp, my_chan = lax.axis_index("dp"), lax.axis_index("chan")
    batch = saved_input.shape[0] * n_dp
    swap, planes = lane_swap(width), to_planes(width)

    share = 2 if own_m % 2 == 0 and n_dp % 2 == 0 else 1
    per = own_m // share
    half_of = my_dp % share
    orders = pick(legendre.reshape(share, per * n_deg, n_lat), half_of)
    by_lat = orders.T.reshape(lat_size, local_lat, per * n_deg)
    by_lat = lax.all_to_all(by_lat, "lat", split_axis=0, concat_axis=0, tiled=True)
    held = [by_lat]
    if share == 2:
        other = lax.ppermute(by_lat, "dp", [(i, i ^ 1) for i in range(n_dp)])
        first = half_of == 0
        held = [jnp.where(first, by_lat, other), jnp.where(first, other, by_lat)]
    held = [
        jnp.transpose(x.reshape(lat_size, local_lat, per, n_deg), (0, 2, 3, 1))
        for x in held
    ]
    table = jnp.concatenate(held, axis=1).reshape(lat_size * own_m, n_deg, local_lat)
    weights = lax.dynamic_slice_in_dim(
        quad_weight, lax.axis_index("lat") * local_lat, local_lat
    )
    analysis = (table.astype(F32) * weights[None, None, :]).astype(BF)

    def spectrum(tab, grid):
        part = jnp.einsum("mlj,bmjq->lbmq", tab, grid, preferred_element_type=F32)
        return lax.psum_scatter(part.astype(BF), "lat", scatter_dimension=0, tiled=True)

    grads = spectrum(table, grad_output)
    spectra = spectrum(analysis, saved_input)
    n_l, n_b, n_m = grads.shape[:3]
    rows = n_b * n_m

    flat = grads.reshape(n_l, rows, width)
    both = jnp.concatenate([flat, lanes(flat, swap)], axis=1)
    n_i = mixing_weight.shape[1]
    mine = n_i // n_chan
    split_weight = mixing_weight.reshape(n_l, n_chan, mine, width)
    terms = jnp.einsum("lrq,lciq->clri", both, split_weight, preferred_element_type=F32)
    terms = terms.astype(BF)
    total = pick(terms, my_chan).astype(F32)
    for step in range(1, n_chan):
        sent = pick(terms, (my_chan + step) % n_chan)
        total = total + shifted(sent, "chan", step).astype(F32)
    total = total.astype(BF)
    half = lanes_join(total.reshape(n_l, 2, rows, mine), planes)
    everyone = [flat] + [shifted(flat, "dp", step) for step in range(1, n_dp)]

    spectra, half, *everyone = lax.optimization_barrier((spectra, half, *everyone))
    spec_in = lax.all_gather(half, "lat", axis=0, tiled=True).reshape(-1, n_b, n_m, width)
    grad_input = jnp.einsum(
        "mlj,lbmq->bmjq", analysis, spec_in, preferred_element_type=F32
    ).astype(BF)

    block = n_i // n_dp
    size = min(block, mine)
    per_chan, per_block = mine // size, block // size
    planar = lanes(spectra.reshape(n_l, rows, width), planes)
    pieces = jnp.moveaxis(planar.reshape(n_l, rows, 2, per_chan, size), 3, 0)
    pieces = pieces.reshape(per_chan, n_l, rows, 2 * size)
    pieces = jnp.concatenate(
        [pieces] + [shifted(pieces, "chan", step) for step in range(1, n_chan)]
    )

    def piece(index):
        place = (my_chan - index // per_chan) % n_chan
        return pick(pieces, place * per_chan + index % per_chan)

    def block_of(owner):
        parts = [piece(owner * per_block + t) for t in range(per_block)]
        return jnp.stack(parts)

    ours = [block_of(my_dp)]
    for step in range(1, n_dp):
        ours.append(shifted(block_of((my_dp + step) % n_dp), "dp", step))
    left = jnp.stack(ours).reshape(n_dp, per_block, n_l, rows, 2, size)
    right = jnp.stack(everyone)
    right = jnp.stack([right, lanes(right, swap)])
    grad_weight = jnp.einsum(
        "dtlrpi,pdlrq->ltiq", left, right, preferred_element_type=F32
    ) / batch
    return (grad_weight.reshape(n_l, block, width).astype(BF), grad_input)


def lanes_join(parts, planes):
    n = parts.shape[-1]
    real = jnp.einsum("lri,qi->lrq", parts[:, 0], planes[:, :n], preferred_element_type=F32)
    imag = jnp.einsum("lri,qi->lrq", parts[:, 1], planes[:, n:], preferred_element_type=F32)
    return (real + imag).astype(BF)


def on_slice(saved_input, grad_output, legendre, quad_weight, mixing_weight):
    n_b, n_m, n_j, width = saved_input.shape
    own_m, n_deg, _ = legendre.shape
    lat, n_dp, n_chan = (lax.axis_size(a) for a in ("lat", "dp", "chan"))
    n_l, n_i, _ = mixing_weight.shape
    fits = (
        n_b == 1 and n_chan == 2 and n_dp % 2 == 0 and n_dp // n_chan == 2
        and n_m == lat * own_m and n_m == 16 and own_m % (2 * n_chan) == 0
        and n_l % 16 == 0 and n_l >= 32 and width % 512 == 0 and n_i == width
        and n_j % 12 == 0
    )
    step = fast if fits else on_device
    return step(saved_input, grad_output, legendre, quad_weight, mixing_weight)


def solution(mesh):
    in_specs = (
        P("dp", None, "lat", "chan"),
        P("dp", None, "lat", "chan"),
        P("lat", None, None),
        P(),
        P("lat", None, "chan"),
    )
    out_specs = (P("lat", "dp", "chan"), P("dp", None, "lat", "chan"))
    return jax.shard_map(
        on_slice, mesh=mesh, in_specs=in_specs, out_specs=out_specs, check_vma=False
    )
```

```python
import functools
import jax
import jax.numpy as jnp
from jax import lax
from jax.experimental import pallas as pl
from jax.experimental.pallas import tpu as pltpu
from jax.sharding import PartitionSpec as P

BF = jnp.bfloat16
F32 = jnp.float32
MESH = pl.DeviceIdType.MESH


START = 0
DELAY = 3


def loop(n, body, unroll=1):
    if n % unroll:
        unroll = 1

    def some(i, carry):
        for j in range(unroll):
            body(i * unroll + j)
        return carry

    lax.fori_loop(0, n // unroll, some, 0)


def nn(a, b):
    return lax.dot_general(a, b, (((1,), (0,)), ((), ())), preferred_element_type=F32)


def nt(a, b):
    return lax.dot_general(a, b, (((1,), (1,)), ((), ())), preferred_element_type=F32)


def tn(a, b):
    return lax.dot_general(a, b, (((0,), (0,)), ((), ())), preferred_element_type=F32)


def put(ref, at, value):
    for i in range(ref.shape[0]):
        ref[i, at, :] = value[:, i * 128:(i + 1) * 128]


def take(ref, start, size, stride):
    at = pl.ds(start, size, stride=stride)
    return jnp.concatenate([ref[i, at, :].astype(BF) for i in range(ref.shape[0])], axis=1)


def partner_rows(x):
    width = x.shape[-1]
    lane = lax.broadcasted_iota(jnp.int32, x.shape, 1)
    ahead, behind = pltpu.roll(x, width - 1, 1), pltpu.roll(x, 1, 1)
    return jnp.where(lane % 2 == 0, ahead, -behind)


def layer_kernel(
    dims,
    leg_hbm, quad_hbm, g_hbm, x_hbm, w_hbm,
    gi_hbm, e_hbm, l_hbm,
    leg, tab, quad_in, quad, raw, wide, table, pg, ps, rgp, rgm, rsp, rsm,
    tall, turned, flat, keep, give, got, spec, planar, rows16, wbuf, split, join, outb,
    load_sem, w_sem, zs_sem, zr_sem, xs_sem, xr_sem, cs_sem, cr_sem,
    gps, gpr, gms, gmr, sps, spr, sms, smr,
    ts_sem, tr_sem, aps, apr, ams, amr, es_sem, er_sem, el_sem, ps_sem, pr_sem, pl_sem, out_sem,
):
    J, M, Q, L, LB, OM, Z, NDP, NCH, K, KB, WL, WS = dims
    half = Q // 2
    z, c, d = lax.axis_index("lat"), lax.axis_index("chan"), lax.axis_index("dp")
    core = d % 2
    mate, other = d + 1 - 2 * core, 1 - c
    per = OM // (2 * NCH)

    def load(src, dst, i):
        return pltpu.make_async_copy(src, dst, load_sem.at[i])

    loads = [load(leg_hbm, leg, 0), load(g_hbm, raw.at[0], 1), load(x_hbm, raw.at[1], 2),
             load(quad_hbm, quad_in, 3)]
    for i in (0, 1, 3, 2):
        loads[i].start()

    def w_copy(i, slot):
        return pltpu.make_async_copy(w_hbm.at[pl.ds(i * WL, WL)], wbuf.at[slot], w_sem.at[slot])

    for i in range(WS):
        w_copy(i, i).start()

    barrier = pltpu.get_barrier_semaphore()
    for i in range(1, Z):
        pl.semaphore_signal(barrier, inc=1, device_id={"lat": (z + i) % Z}, device_id_type=MESH)
    for i in range(NDP):
        for j in range(NCH):
            if i or j:
                pl.semaphore_signal(
                    barrier, inc=1, device_id={"dp": (d + i) % NDP, "chan": (c + j) % NCH},
                    device_id_type=MESH)

    loads[0].wait()

    def cut(i):
        whole = leg[i]
        for t in range(Z):
            tab[t, i] = whole[:, t * J:(t + 1) * J]

    loop(OM, cut)

    def own_table(i):
        table[z * OM + i] = tab[z, i]

    loop(OM, own_table)
    loads[1].wait()
    JB = 12 if J % 12 == 0 else 1

    def spread(which):
        def body(i):
            block = raw[which, pl.ds(i * JB, JB)]
            put(wide, pl.ds(i * JB * M, JB * M), block.astype(F32).reshape(JB * M, Q))
        loop(J // JB, body)

    def rows_of(m):
        return take(wide, m, J, M)

    spread(0)

    def grad_part(m):
        pg[m] = nn(table[m], rows_of(m)).astype(BF)

    pl.semaphore_wait(barrier, Z - 1 + NDP * NCH - 1)

    mine_q = c * 2 + core

    def z_copy(target, source):
        return pltpu.make_async_remote_copy(
            src_ref=tab.at[target, pl.ds(mine_q * per, per)],
            dst_ref=table.at[pl.ds(source * OM + mine_q * per, per)],
            send_sem=zs_sem.at[target], recv_sem=zr_sem.at[source],
            device_id={"lat": target}, device_id_type=MESH)

    def quarter(owner, q, sends, recvs, where):
        part = table.at[pl.ds(owner * OM + q * per, per)]
        return pltpu.make_async_remote_copy(
            src_ref=part, dst_ref=part, send_sem=sends, recv_sem=recvs,
            device_id=where, device_id_type=MESH)

    def line_steps(p, rp, rm, sends_p, recvs_p, sends_m, recvs_m, region):
        def copy_p(s, t):
            r = region(s, t)
            return pltpu.make_async_remote_copy(
                src_ref=p.at[r], dst_ref=rp.at[r], send_sem=sends_p.at[s, t],
                recv_sem=recvs_p.at[s, t], device_id={"lat": (z + 1) % Z}, device_id_type=MESH)

        def copy_m(s, t):
            r = region(s, t)
            return pltpu.make_async_remote_copy(
                src_ref=p.at[r], dst_ref=rm.at[r], send_sem=sends_m.at[s, t],
                recv_sem=recvs_m.at[s, t], device_id={"lat": (z + Z - 1) % Z}, device_id_type=MESH)

        return copy_p, copy_m

    def g_region(s, t):
        return (pl.ds(s * OM, OM), pl.ds(t * LB, LB), slice(None))

    def s_region(k, t):
        return (slice(None), pl.ds(t * LB + k * KB, KB), slice(None))

    g_p, g_m = line_steps(pg, rgp, rgm, gps, gpr, gms, gmr, g_region)
    s_p, s_m = line_steps(ps, rsp, rsm, sps, spr, sms, smr, s_region)

    def add_g(r, s, t):
        def body(i):
            at = (s * OM + i, pl.ds(t * LB, LB), slice(None))
            pg[at] = (pg[at].astype(F32) + r[at].astype(F32)).astype(BF)
        loop(OM, body)

    def add_s(r, k, t):
        def body(i):
            at = (i, pl.ds(t * LB + k * KB, KB), slice(None))
            ps[at] = (ps[at].astype(F32) + r[at].astype(F32)).astype(BF)
        loop(M, body)

    first, last = z == 0, z == Z - 1

    for i in range(1, Z):
        z_copy((z + Z - i) % Z, z).start()
    loop(OM, lambda i: grad_part(z * OM + i))

    @pl.when(first)
    def _():
        for t in [*range(Z - 2, 0, -1), Z - 1]:
            g_p(0, t).start()

    @pl.when(last)
    def _():
        for t in [*range(1, Z - 1), 0]:
            g_m(Z - 1, t).start()

    def from_line(i):
        source = (z + i) % Z
        z_copy(z, source).wait_recv()
        quarter(source, mine_q, xs_sem.at[source], xr_sem.at[source], {"chan": other}).start()
        quarter(source, mine_q, cs_sem.at[source, 0], cr_sem.at[source, 0], {"dp": mate}).start()

    def from_side(i):
        source = (z + i) % Z
        x_q = other * 2 + core
        quarter(source, x_q, xs_sem.at[source], xr_sem.at[source], {"chan": other}).wait_recv()
        quarter(source, x_q, cs_sem.at[source, 1], cr_sem.at[source, 1], {"dp": mate}).start()

    def from_mate(i):
        source = (z + i) % Z
        quarter(source, c * 2 + 1 - core, cs_sem.at[source, 0], cr_sem.at[source, 0], {"dp": mate}).wait_recv()
        quarter(source, other * 2 + 1 - core, cs_sem.at[source, 1], cr_sem.at[source, 1], {"dp": mate}).wait_recv()
        loop(OM, lambda m: grad_part(source * OM + m))

    for i in range(1, Z + 2):
        if i < Z:
            from_line(i)
        if 1 < i < Z + 1:
            from_side(i - 1)
        if i > 2:
            from_mate(i - 2)

    def clear(r):
        def body(i):
            r[i, pl.ds(z * LB, LB), :] = jnp.zeros((LB, Q), BF)
        loop(M, body)

    @pl.when(first)
    def _():
        clear(rgp)
        clear(rsp)

    @pl.when(last)
    def _():
        clear(rgm)
        clear(rsm)

    def order(u):
        v = u - (Z - 1)
        early = u < Z - 1
        p = jnp.where(early, u, v // (Z - 1))
        return jnp.where(early, 0, 1 + v % (Z - 1)), jnp.where(p < Z - 2, Z - 2 - p, Z - 1)

    def down_block(t):
        return Z - 1 - t

    pieces = Z * (Z - 1)

    def g_ends(u):
        s, t = order(u)

        @pl.when(first)
        def _():
            g_p(s, t).start()

        @pl.when(last)
        def _():
            g_m(Z - 1 - s, down_block(t)).start()

    lax.fori_loop(Z - 1, pieces, lambda u, v: (g_ends(u), v)[1], 0)

    loads[2].wait()
    loads[3].wait()
    weights = quad_in[...].reshape(1, Z * J)
    for t in range(Z):
        quad[t:t + 1, :] = weights[:, t * J:(t + 1) * J]

    spread(1)

    def input_part(m):
        tall[m] = (table[m].astype(F32) * quad[pl.ds(z, 1), :]).astype(BF)
        ps[m] = nn(tall[m], rows_of(m)).astype(BF)

    loop(M, input_part, 2)

    def s_send(k):
        @pl.when(first)
        def _():
            for t in range(Z - 1, 0, -1):
                s_p(k, t).start()

        @pl.when(last)
        def _():
            for t in range(Z - 1):
                s_m(k, t).start()

    for k in range(K - 1):
        s_send(k)

    def g_done(s):
        @pl.when(z > 0)
        def _():
            g_p(s, z).wait_recv()

        @pl.when(z < Z - 1)
        def _():
            g_m(s, z).wait_recv()

    row = lax.broadcasted_iota(jnp.int32, (Q, Q), 0)
    col = lax.broadcasted_iota(jnp.int32, (Q, Q), 1)
    side = half // (NDP // NCH)
    chan, part = row // 2, row % 2
    split[...] = jnp.where((chan // side) * 2 * side + part * side + chan % side == col, 1.0, 0.0).astype(BF)
    for i in range(2):
        join[i] = jnp.where(2 * row[:half] + i == col[:half], 1.0, 0.0).astype(BF)

    def sum_g(m):
        at = (m, pl.ds(z * LB, LB), slice(None))
        put(wide, pl.ds(m * LB, LB), pg[at].astype(F32) + rgp[at].astype(F32) + rgm[at].astype(F32))


    def flat_of(l):
        rows = take(wide, l, M, LB)
        flat[l, :M, :] = rows
        flat[l, M:, :] = partner_rows(rows.astype(F32)).astype(BF)


    def e_copy(i):
        return pltpu.make_async_remote_copy(
            src_ref=flat.at[:, pl.ds(0, M)], dst_ref=e_hbm.at[d], send_sem=es_sem.at[i],
            recv_sem=er_sem.at[d], device_id={"dp": (d + i) % NDP}, device_id_type=MESH)

    def e_recv(b):
        return pltpu.make_async_remote_copy(
            src_ref=flat.at[:, pl.ds(0, M)], dst_ref=e_hbm.at[b], send_sem=es_sem.at[0],
            recv_sem=er_sem.at[b], device_id={"dp": mate}, device_id_type=MESH)

    e_local = pltpu.make_async_copy(flat.at[:, pl.ds(0, M)], e_hbm.at[d], el_sem.at[0])

    def own_spectra():
        loop(Z, g_done)
        loop(M, sum_g, 2)
        loop(LB, flat_of, 4)
        e_local.start()
        for i in range(1, NDP):
            e_copy(i).start()

    def t_copy(k):
        rows = pl.ds(k * KB, KB)
        return pltpu.make_async_remote_copy(
            src_ref=give.at[rows], dst_ref=got.at[rows], send_sem=ts_sem.at[k],
            recv_sem=tr_sem.at[k], device_id={"chan": other}, device_id_type=MESH)

    def mix(i):
        slot = i % WS
        w_copy(i, slot).wait()

        def one(j):
            l = i * WL + j
            both = flat[l]
            give[l] = nt(both, wbuf[slot, j, pl.ds(other * half, half), :]).astype(BF)
            keep[l] = nt(both, wbuf[slot, j, pl.ds(c * half, half), :]).astype(BF)

        loop(WL, one)

        @pl.when(i + WS < LB // WL)
        def _():
            w_copy(i + WS, slot).start()

        done = (i + 1) * WL

        @pl.when(done % KB == 0)
        def _():
            t_copy(done // KB - 1).start()

    owners = NDP // NCH
    piece_width = Q // owners

    def p_copy(k, e, j):
        return pltpu.make_async_remote_copy(
            src_ref=planar.at[pl.ds(k * KB, KB), :, pl.ds(e * piece_width, piece_width)],
            dst_ref=l_hbm.at[d, pl.ds(k * KB, KB)],
            send_sem=ps_sem.at[k, e * NCH + j], recv_sem=pr_sem.at[k, d],
            device_id={"dp": c * owners + e, "chan": j}, device_id_type=MESH)

    def p_recv(k, b):
        return pltpu.make_async_remote_copy(
            src_ref=planar.at[pl.ds(k * KB, KB), :, pl.ds(0, piece_width)],
            dst_ref=l_hbm.at[b, pl.ds(k * KB, KB)],
            send_sem=ps_sem.at[k, 0], recv_sem=pr_sem.at[k, b],
            device_id={"dp": mate}, device_id_type=MESH)

    def p_local(k, e):
        return pltpu.make_async_copy(
            planar.at[pl.ds(k * KB, KB), :, pl.ds(e * piece_width, piece_width)],
            l_hbm.at[d, pl.ds(k * KB, KB)], pl_sem.at[k])

    def is_me(e, j):
        return (d == c * owners + e) & (c == j)

    def s_finish(k):
        @pl.when(z > 0)
        def _():
            s_p(k, z).wait_recv()

        @pl.when(z < Z - 1)
        def _():
            s_m(k, z).wait_recv()

        def total(m):
            at = (m, pl.ds(z * LB + k * KB, KB), slice(None))
            put(wide, pl.ds(m * KB, KB), ps[at].astype(F32) + rsp[at].astype(F32) + rsm[at].astype(F32))

        loop(M, total, 2)

        def one(l):
            rows16[pl.ds(l * M, M), :] = take(wide, l, M, KB)

        loop(KB, one, 4)
        planar[pl.ds(k * KB, KB)] = nn(rows16[...], split[...]).astype(BF).reshape(KB, M, Q)
        for e in range(owners):
            for j in range(NCH):
                @pl.when(is_me(e, j))
                def _():
                    p_local(k, e).start()

                @pl.when(jnp.logical_not(is_me(e, j)))
                def _():
                    p_copy(k, e, j).start()

    def a_region(t, k):
        return (slice(None), pl.ds(t * LB + k * KB, KB), slice(None))

    def a_p(t, k):
        part = spec.at[a_region(t, k)]
        return pltpu.make_async_remote_copy(
            src_ref=part, dst_ref=part, send_sem=aps.at[t, k], recv_sem=apr.at[t, k],
            device_id={"lat": (z + 1) % Z}, device_id_type=MESH)

    def a_m(t, k):
        part = spec.at[a_region(t, k)]
        return pltpu.make_async_remote_copy(
            src_ref=part, dst_ref=part, send_sem=ams.at[t, k], recv_sem=amr.at[t, k],
            device_id={"lat": (z + Z - 1) % Z}, device_id_type=MESH)

    def combine(k):
        t_copy(k).wait_recv()
        rows = pl.ds(k * KB, KB)
        total = (keep[rows].astype(F32) + got[rows].astype(F32)).astype(BF)
        real = total[:, :M].reshape(KB * M, half)
        imag = total[:, M:].reshape(KB * M, half)
        put(wide, pl.ds(0, KB * M), nn(real, join[0]) + nn(imag, join[1]))

        def one(m):
            spec[m, pl.ds(z * LB + k * KB, KB), :] = take(wide, m, KB, M)

        loop(M, one, 4)

        @pl.when(z < Z - 1)
        def _():
            a_p(z, k).start()

        @pl.when(z > 0)
        def _():
            a_m(z, k).start()

        @pl.when(k == K - 1)
        def _():
            s_send(K - 1)

    def mix_rows(k):
        lax.fori_loop(k * (KB // WL), (k + 1) * (KB // WL), lambda i, v: (mix(i), v)[1], 0)

    s_count = (K - 1) * (Z - 1)
    gather_at = pieces + s_count
    final_at = gather_at + K
    total_pieces = final_at + Z - 1

    def up(n):
        @pl.when((n >= 0) & (n < pieces))
        def _():
            s, t = order(n)

            @pl.when(t > z)
            def _():
                g_p(s, t).wait_recv()
                add_g(rgp, s, t)
                g_p(s, t).start()

        late = n >= final_at

        @pl.when(((n >= pieces) & (n < gather_at)) | (late & (n < total_pieces)))
        def _():
            v = jnp.where(late, n - final_at + s_count, n - pieces)
            k, t = v // (Z - 1), Z - 1 - v % (Z - 1)

            @pl.when(t > z)
            def _():
                s_p(k, t).wait_recv()
                add_s(rsp, k, t)
                s_p(k, t).start()

        @pl.when((n >= gather_at) & (n < final_at))
        def _():
            a_p(0, n - gather_at).wait_recv()
            a_p(0, n - gather_at).start()

    def down(n):
        @pl.when((n >= 0) & (n < pieces))
        def _():
            s, t = order(n)
            s, t = Z - 1 - s, down_block(t)

            @pl.when(t < z)
            def _():
                g_m(s, t).wait_recv()
                add_g(rgm, s, t)
                g_m(s, t).start()

        late = n >= final_at

        @pl.when(((n >= pieces) & (n < gather_at)) | (late & (n < total_pieces)))
        def _():
            v = jnp.where(late, n - final_at + s_count, n - pieces)
            k, t = v // (Z - 1), v % (Z - 1)

            @pl.when(t < z)
            def _():
                s_m(k, t).wait_recv()
                add_s(rsm, k, t)
                s_m(k, t).start()

        @pl.when((n >= gather_at) & (n < final_at))
        def _():
            a_m(Z - 1, n - gather_at).wait_recv()
            a_m(Z - 1, n - gather_at).start()

    inner = jnp.logical_not(first | last)
    begin = (Z - 1) * (Z - 1) + START - 1
    ready = [pieces + (k + 1) * (Z - 1) + 2 for k in range(K - 1)]

    low_half, high_half = inner & (2 * z < Z - 1), inner & (2 * z >= Z - 1)
    turn = begin + K + 2

    def flip(m):
        turned[m] = tall[m].T

    def slot(v):
        u = v - begin

        @pl.when(u == 0)
        def _():
            own_spectra()

        @pl.when((u >= 1) & (u < K + 1))
        def _():
            mix_rows(u - 1)

        @pl.when(u == K + 2)
        def _():
            combine(K - 1)

        early = v < turn

        @pl.when(low_half & early)
        def _():
            down(v - (Z - 2 - z))

        @pl.when(high_half & early)
        def _():
            up(v - (z - 1))

        @pl.when(u == K + 1)
        def _():
            loop(K - 1, combine)

        @pl.when(low_half)
        def _():
            up(v - (z - 1))

        @pl.when(high_half)
        def _():
            down(v - (Z - 2 - z))

        for b in range(1, Z - 1):
            @pl.when((b < z) & inner)
            def _():
                w = v - begin - (K - 1) - DELAY * (z - b)

                @pl.when((w >= 0) & (w < K))
                def _():
                    a_p(b, w).wait_recv()
                    a_p(b, w).start()

            @pl.when((b > z) & inner)
            def _():
                w = v - begin - (K - 1) - DELAY * (b - z)

                @pl.when((w >= 0) & (w < K))
                def _():
                    a_m(b, w).wait_recv()
                    a_m(b, w).start()

        @pl.when(low_half & (v > turn))
        def _():
            down(v - 1 - (Z - 2 - z))

        @pl.when(high_half & (v > turn))
        def _():
            up(v - 1 - (z - 1))

        @pl.when(v == begin + K + 3)
        def _():
            loop(M, flip, 2)

        hit = functools.reduce(lambda a, b: a | b, [v == r for r in ready])

        @pl.when(hit)
        def _():
            s_finish((v - ready[0]) // (Z - 1))

    loop(total_pieces + Z - 1, slot)

    def collect(i):
        b, k = i // K, i % K

        @pl.when(last & (b < Z - 1))
        def _():
            a_p(b, k).wait_recv()

        @pl.when(first & (b > 0))
        def _():
            a_m(b, k).wait_recv()

    s_finish(K - 1)
    loop(Z * K, collect)

    def back(m):
        put(wide, pl.ds(m, J, stride=M), nn(turned[m], spec[m]))

    loop(M, back, 2)

    def narrow(i):
        at = pl.ds(i * JB, JB)
        rows = pl.ds(i * JB * M, JB * M)
        for q in range(Q // 128):
            outb[at, :, q * 128:(q + 1) * 128] = wide[q, rows, :].reshape(JB, M, 128).astype(BF)

    parts = 3 if J % (3 * JB) == 0 else 1

    def out(i):
        rows = pl.ds(i * (J // parts), J // parts)
        return pltpu.make_async_copy(outb.at[rows], gi_hbm.at[rows], out_sem.at[i])

    for i in range(parts):
        each = J // JB // parts
        lax.fori_loop(i * each, (i + 1) * each, lambda j, v: (narrow(j), v)[1], 0)
        out(i).start()
    e_local.wait()
    for i in range(1, NDP):
        e_copy(i).wait_send()
        e_recv((d + i) % NDP).wait_recv()
    for k in range(K):
        t_copy(k).wait_send()
        for e in range(owners):
            for j in range(NCH):
                @pl.when(is_me(e, j))
                def _():
                    p_local(k, e).wait()

                @pl.when(jnp.logical_not(is_me(e, j)))
                def _():
                    p_copy(k, e, j).wait_send()
        for b in range(NDP):
            @pl.when(jnp.logical_not((b == d) & (d // owners == c)))
            def _():
                p_recv(k, b).wait_recv()
    for i in range(1, Z):
        source = (z + i) % Z
        z_copy(source, z).wait_send()
        quarter(source, mine_q, xs_sem.at[source], xr_sem.at[source], {"chan": other}).wait_send()
        quarter(source, mine_q, cs_sem.at[source, 0], cr_sem.at[source, 0], {"dp": mate}).wait_send()
        quarter(source, other * 2 + core, cs_sem.at[source, 1], cr_sem.at[source, 1], {"dp": mate}).wait_send()

    def drain_line(i):
        s, t = i // Z, i % Z

        @pl.when((t > z) & (z < Z - 1))
        def _():
            g_p(s, t).wait_send()

        @pl.when((t < z) & (z > 0))
        def _():
            g_m(s, t).wait_send()

    loop(Z * Z, drain_line)

    def drain_rest(i):
        k, t = i // Z, i % Z

        @pl.when(t > z)
        def _():
            s_p(k, t).wait_send()

        @pl.when(t < z)
        def _():
            s_m(k, t).wait_send()

        @pl.when((t <= z) & (z < Z - 1))
        def _():
            a_p(t, k).wait_send()

        @pl.when((t >= z) & (z > 0))
        def _():
            a_m(t, k).wait_send()

    loop(K * Z, drain_rest)
    for i in range(parts):
        out(i).wait()


def weight_kernel(scale, e_ref, l_ref, out_ref):
    n_b, n_l, m, q = e_ref.shape
    side = l_ref.shape[-1] // 2

    for l in range(n_l):
        right = e_ref[:, l].reshape(n_b * m, q)
        left = l_ref[:, l].reshape(n_b * m, 2 * side)
        turned = partner_rows(right.astype(F32)).astype(BF)
        total = tn(jnp.concatenate([left[:, :side], left[:, side:]], axis=0),
                   jnp.concatenate([right, turned], axis=0))
        out_ref[l] = (total * scale).astype(BF)


def fast(saved_input, grad_output, legendre, quad_weight, mixing_weight):
    _, M, J, Q = saved_input.shape
    OM, L, _ = legendre.shape
    Z, NDP, NCH = lax.axis_size("lat"), lax.axis_size("dp"), lax.axis_size("chan")
    LB, NI, _ = mixing_weight.shape
    KB = 16
    K = LB // KB
    WL, WS = 8, 3
    half = Q // 2
    owners = NDP // NCH
    side = half // owners
    dims = (J, M, Q, L, LB, OM, Z, NDP, NCH, K, KB, WL, WS)
    quad = quad_weight
    g = jnp.transpose(grad_output[0], (1, 0, 2))
    x = jnp.transpose(saved_input[0], (1, 0, 2))
    anyspec = pl.BlockSpec(memory_space=pl.ANY)
    dma = pltpu.SemaphoreType.DMA
    part_shape = pltpu.VMEM((M, L, Q), BF)
    scratch = [
        pltpu.VMEM((OM, L, Z * J), BF), pltpu.VMEM((Z, OM, L, J), BF), pltpu.VMEM((Z * J,), F32), pltpu.VMEM((Z, J), F32), pltpu.VMEM((2, J, M, Q), BF),
        pltpu.VMEM((Q // 128, J * M, 128), F32), pltpu.VMEM((M, L, J), BF),
        part_shape, part_shape, part_shape, part_shape, part_shape, part_shape,
        pltpu.VMEM((M, L, J), BF), pltpu.VMEM((M, J, L), BF), pltpu.VMEM((LB, 2 * M, Q), BF),
        pltpu.VMEM((LB, 2 * M, half), BF), pltpu.VMEM((LB, 2 * M, half), BF),
        pltpu.VMEM((LB, 2 * M, half), BF), part_shape, pltpu.VMEM((LB, M, Q), BF),
        pltpu.VMEM((KB * M, Q), BF),
        pltpu.VMEM((WS, WL, NI, Q), BF), pltpu.VMEM((Q, Q), BF), pltpu.VMEM((2, half, Q), BF),
        pltpu.VMEM((J, M, Q), BF),
        dma((4,)), dma((WS,)), dma((Z,)), dma((Z,)), dma((Z,)), dma((Z,)), dma((Z, 2)), dma((Z, 2)),
        dma((Z, Z)), dma((Z, Z)), dma((Z, Z)), dma((Z, Z)),
        dma((K, Z)), dma((K, Z)), dma((K, Z)), dma((K, Z)),
        dma((K,)), dma((K,)), dma((Z, K)), dma((Z, K)), dma((Z, K)), dma((Z, K)),
        dma((NDP,)), dma((NDP,)), dma((1,)), dma((K, owners * NCH)), dma((K, NDP)), dma((K,)),
        dma((3,)),
    ]
    gi, e, left = pl.pallas_call(
        functools.partial(layer_kernel, dims),
        out_shape=(
            jax.ShapeDtypeStruct((J, M, Q), BF),
            jax.ShapeDtypeStruct((NDP, LB, M, Q), BF),
            jax.ShapeDtypeStruct((NDP, LB, M, 2 * side), BF),
        ),
        in_specs=[anyspec] * 5,
        out_specs=(anyspec,) * 3,
        scratch_shapes=scratch,
        compiler_params=pltpu.CompilerParams(
            collective_id=0, has_side_effects=True, vmem_limit_bytes=67043328
        ),
        name="layer",
    )(legendre, quad, g, x, mixing_weight)
    WB = 16
    gw = pl.pallas_call(
        functools.partial(weight_kernel, 1.0 / (NDP * saved_input.shape[0])),
        out_shape=jax.ShapeDtypeStruct((LB, side, Q), BF),
        grid=(LB // WB,),
        in_specs=[
            pl.BlockSpec((NDP, WB, M, Q), lambda i: (0, i, 0, 0)),
            pl.BlockSpec((NDP, WB, M, 2 * side), lambda i: (0, i, 0, 0)),
        ],
        out_specs=pl.BlockSpec((WB, side, Q), lambda i: (i, 0, 0)),
        compiler_params=pltpu.CompilerParams(dimension_semantics=("arbitrary",)),
        name="weight",
    )(e, left)
    return gw, jnp.transpose(gi, (1, 0, 2))[None]


def lane_swap(width):
    row = lax.broadcasted_iota(jnp.int32, (width, width), 0)
    col = lax.broadcasted_iota(jnp.int32, (width, width), 1)
    up = (row == col + 1) & (col % 2 == 0)
    down = (col == row + 1) & (row % 2 == 0)
    return (up.astype(F32) - down.astype(F32)).astype(BF)


def to_planes(width):
    row = lax.broadcasted_iota(jnp.int32, (width, width), 0)
    col = lax.broadcasted_iota(jnp.int32, (width, width), 1)
    return ((row // 2 + (row % 2) * (width // 2)) == col).astype(BF)


def lanes(x, matrix):
    return jnp.einsum("...q,qp->...p", x, matrix, preferred_element_type=F32).astype(BF)


def shifted(x, axis, step):
    n = lax.axis_size(axis)
    return lax.ppermute(x, axis, [(i, (i + step) % n) for i in range(n)])


def pick(x, index):
    return lax.dynamic_index_in_dim(x, index, 0, keepdims=False)


def on_device(saved_input, grad_output, legendre, quad_weight, mixing_weight):
    local_lat = saved_input.shape[2]
    width = saved_input.shape[3]
    own_m, n_deg, n_lat = legendre.shape
    lat_size = lax.axis_size("lat")
    n_dp, n_chan = lax.axis_size("dp"), lax.axis_size("chan")
    my_dp, my_chan = lax.axis_index("dp"), lax.axis_index("chan")
    batch = saved_input.shape[0] * n_dp
    swap, planes = lane_swap(width), to_planes(width)

    share = 2 if own_m % 2 == 0 and n_dp % 2 == 0 else 1
    per = own_m // share
    half_of = my_dp % share
    orders = pick(legendre.reshape(share, per * n_deg, n_lat), half_of)
    by_lat = orders.T.reshape(lat_size, local_lat, per * n_deg)
    by_lat = lax.all_to_all(by_lat, "lat", split_axis=0, concat_axis=0, tiled=True)
    held = [by_lat]
    if share == 2:
        other = lax.ppermute(by_lat, "dp", [(i, i ^ 1) for i in range(n_dp)])
        first = half_of == 0
        held = [jnp.where(first, by_lat, other), jnp.where(first, other, by_lat)]
    held = [
        jnp.transpose(x.reshape(lat_size, local_lat, per, n_deg), (0, 2, 3, 1))
        for x in held
    ]
    table = jnp.concatenate(held, axis=1).reshape(lat_size * own_m, n_deg, local_lat)
    weights = lax.dynamic_slice_in_dim(
        quad_weight, lax.axis_index("lat") * local_lat, local_lat
    )
    analysis = (table.astype(F32) * weights[None, None, :]).astype(BF)

    def spectrum(tab, grid):
        part = jnp.einsum("mlj,bmjq->lbmq", tab, grid, preferred_element_type=F32)
        return lax.psum_scatter(part.astype(BF), "lat", scatter_dimension=0, tiled=True)

    grads = spectrum(table, grad_output)
    spectra = spectrum(analysis, saved_input)
    n_l, n_b, n_m = grads.shape[:3]
    rows = n_b * n_m

    flat = grads.reshape(n_l, rows, width)
    both = jnp.concatenate([flat, lanes(flat, swap)], axis=1)
    n_i = mixing_weight.shape[1]
    mine = n_i // n_chan
    split_weight = mixing_weight.reshape(n_l, n_chan, mine, width)
    terms = jnp.einsum("lrq,lciq->clri", both, split_weight, preferred_element_type=F32)
    terms = terms.astype(BF)
    total = pick(terms, my_chan).astype(F32)
    for step in range(1, n_chan):
        sent = pick(terms, (my_chan + step) % n_chan)
        total = total + shifted(sent, "chan", step).astype(F32)
    total = total.astype(BF)
    half = lanes_join(total.reshape(n_l, 2, rows, mine), planes)
    everyone = [flat] + [shifted(flat, "dp", step) for step in range(1, n_dp)]

    spectra, half, *everyone = lax.optimization_barrier((spectra, half, *everyone))
    spec_in = lax.all_gather(half, "lat", axis=0, tiled=True).reshape(-1, n_b, n_m, width)
    grad_input = jnp.einsum(
        "mlj,lbmq->bmjq", analysis, spec_in, preferred_element_type=F32
    ).astype(BF)

    block = n_i // n_dp
    size = min(block, mine)
    per_chan, per_block = mine // size, block // size
    planar = lanes(spectra.reshape(n_l, rows, width), planes)
    pieces = jnp.moveaxis(planar.reshape(n_l, rows, 2, per_chan, size), 3, 0)
    pieces = pieces.reshape(per_chan, n_l, rows, 2 * size)
    pieces = jnp.concatenate(
        [pieces] + [shifted(pieces, "chan", step) for step in range(1, n_chan)]
    )

    def piece(index):
        place = (my_chan - index // per_chan) % n_chan
        return pick(pieces, place * per_chan + index % per_chan)

    def block_of(owner):
        parts = [piece(owner * per_block + t) for t in range(per_block)]
        return jnp.stack(parts)

    ours = [block_of(my_dp)]
    for step in range(1, n_dp):
        ours.append(shifted(block_of((my_dp + step) % n_dp), "dp", step))
    left = jnp.stack(ours).reshape(n_dp, per_block, n_l, rows, 2, size)
    right = jnp.stack(everyone)
    right = jnp.stack([right, lanes(right, swap)])
    grad_weight = jnp.einsum(
        "dtlrpi,pdlrq->ltiq", left, right, preferred_element_type=F32
    ) / batch
    return (grad_weight.reshape(n_l, block, width).astype(BF), grad_input)


def lanes_join(parts, planes):
    n = parts.shape[-1]
    real = jnp.einsum("lri,qi->lrq", parts[:, 0], planes[:, :n], preferred_element_type=F32)
    imag = jnp.einsum("lri,qi->lrq", parts[:, 1], planes[:, n:], preferred_element_type=F32)
    return (real + imag).astype(BF)


def on_slice(saved_input, grad_output, legendre, quad_weight, mixing_weight):
    n_b, n_m, n_j, width = saved_input.shape
    own_m, n_deg, _ = legendre.shape
    lat, n_dp, n_chan = (lax.axis_size(a) for a in ("lat", "dp", "chan"))
    n_l, n_i, _ = mixing_weight.shape
    fits = (
        n_b == 1 and n_chan == 2 and n_dp % 2 == 0 and n_dp // n_chan == 2
        and n_m == lat * own_m and n_m == 16 and own_m % (2 * n_chan) == 0
        and n_l % 16 == 0 and n_l >= 32 and width % 512 == 0 and n_i == width
        and n_j % 12 == 0
    )
    step = fast if fits else on_device
    return step(saved_input, grad_output, legendre, quad_weight, mixing_weight)


def solution(mesh):
    in_specs = (
        P("dp", None, "lat", "chan"),
        P("dp", None, "lat", "chan"),
        P("lat", None, None),
        P(),
        P("lat", None, "chan"),
    )
    out_specs = (P("lat", "dp", "chan"), P("dp", None, "lat", "chan"))
    return jax.shard_map(
        on_slice, mesh=mesh, in_specs=in_specs, out_specs=out_specs, check_vma=False
    )
```
